32 devices in a mesh: dp: 4 (over y, core), expert: 8 (over z, x).
Axes of the slice: x: 2, y: 2, z: 4, core: 2. Of those that a mesh axis runs over, the one named last changes fastest.
Arguments:
- hidden: bfloat16 [8192, 768], P(('dp', 'expert')), may hold values from -6 to 6
- w_down: bfloat16 [8, 768, 2048], P('expert', 'dp'), may hold values from -0.21875 to 0.21875
- expert_ids: int32 [1024, 4], P(('dp', 'expert')), may hold values from 0 to 7, all different within a row; in each aligned block of 32 rows (0 to 31, 32 to 63, ...) at most 32 rows name the same one
- gates: float32 [1024, 4], P(('dp', 'expert')), may hold values from 0.05 to 1
- cotangent: bfloat16 [1024, 2048], P(('dp', 'expert')), may hold values from -6 to 6
Outputs:
- mixed: bfloat16 [1024, 2048], P(('dp', 'expert'))
- gate_grads: float32 [1024, 4], P(('dp', 'expert'))
- hidden_grads: bfloat16 [8192, 768], P(('dp', 'expert'))
- weight_grads: bfloat16 [8, 768, 2048], P('expert', 'dp')
The draws below stay inside these ranges and needn't reach their ends.
Inputs may be any that keep to these rules, and one draw needn't show every extreme that they name: `expert_ids`: each row names 4 different experts. Among the rows of one device no expert is named more than 32 times, a bound that some block reaches.
All inputs are finite; a program needn't handle non-finite values.
Results may differ from the reference program's by a relative error of at most 0.015.
Values may be sent and summed in bfloat16 or wider, within the bound.
A program may use at most 64 MiB of HBM per device.

```python
import math
import jax
import jax.numpy as jnp
import numpy as np
from jax import lax

D = 2048
F = 768
TOPK = 4
TOK_DEV = 32
CAP = 32
RECV = 256
EXPERTS = 8
TOKENS = 1024
N_DP = 4
N_EXPERT = 8


def level_of(rng, dims, shards, smallest, high):
    loudness, own = 1.0, jax.random.fold_in(rng, 6)
    for dim, shards_of in shards:
        heights = jnp.exp(jax.random.uniform(jax.random.fold_in(own, dim), (shards_of,), jnp.float32, smallest / len(shards), high / len(shards)))
        loudness = loudness * jnp.repeat(heights, dims[dim] // shards_of).reshape([-1 if axis == dim else 1 for axis in range(len(dims))])
    return loudness


def assign_block(stream_key, own, number, rows, amount, top, reach, slope):
    ranking = jax.random.permutation(stream_key, amount)
    crowded, common = shares(amount, rows * top, reach, slope, True), shares(amount, rows * top, reach, slope, False)
    places = jnp.arange(amount)

    def named(lengths, offset_by):
        used = int((lengths > 0).sum())
        fixed = max(1, used // 4)
        shifted = fixed + (places - fixed + offset_by * (used - fixed)) % max(1, amount - fixed)
        return jnp.zeros((amount,), jnp.int32).at[ranking[jnp.where(places < fixed, places, shifted)]].set(jnp.asarray(lengths, jnp.int32))

    lengths = jnp.where(number % 4 == 0, named(crowded, number // 4), named(common, number - number // 4 - 1))
    mixed = jax.random.permutation(jax.random.fold_in(own, 3), amount)
    giver, receiver = mixed[0:amount // 2 * 2:2], mixed[1:amount // 2 * 2:2]
    room = jnp.minimum(lengths[giver] - 1, reach - lengths[receiver]) // 2
    room = jnp.where((giver == ranking[0]) | (receiver == ranking[0]) | (lengths[receiver] == 0), 0, jnp.maximum(room, 0))
    shifted = jax.random.randint(jax.random.fold_in(own, 4), (amount // 2,), 0, 1 << 20) % (room + 1)
    lengths = lengths.at[giver].add(-shifted).at[receiver].add(shifted)
    labels = jnp.searchsorted(jnp.cumsum(lengths), jnp.arange(rows * top), side="right").astype(jnp.int32)
    table = labels.reshape(top, rows).T
    table = table[jax.random.permutation(jax.random.fold_in(own, 1), rows)]
    offset_by = jax.random.randint(jax.random.fold_in(own, 2), (rows, 1), 0, top)
    return jnp.take_along_axis(table, (jnp.arange(top)[None, :] + offset_by) % top, axis=1)


def shares(amount, total, bound, slope, full):
    portions = [(1 << 20) // math.isqrt(grade ** slope) + 1 for grade in range(1, amount + 1)]
    largest = bound if full else min(bound, max(-(-total // amount), total * portions[0] // sum(portions)))
    least = 1 if total - largest >= amount - 1 else 0
    holding, spare = [largest] + [least] * (amount - 1), total - largest - least * (amount - 1)
    while spare > 0:
        movable = [i for i in range(1, amount) if holding[i] < largest] or [i for i in range(1, amount) if holding[i] < bound]
        mass, left = sum([portions[i] for i in movable]), spare
        for i in movable:
            extra = min(bound - holding[i], max(1, left * portions[i] // mass), spare)
            holding[i] = holding[i] + extra
            spare = spare - extra
    return np.array(holding)


def bell_draw(own_key, shape, deviation, limit, cuts=(), kind=jnp.bfloat16):
    factor_of = level_of(own_key, shape, cuts, -0.22, 0.18) if cuts else 1.0
    result = jax.random.normal(own_key, shape, jnp.float32) * deviation * factor_of
    return jnp.minimum(jnp.maximum(result, -limit), limit).astype(kind)


def setup_inputs(seed: int = 0) -> dict:
    splits = jax.random.split(jax.random.key(seed), 6)
    hidden = bell_draw(splits[0], (N_DP * N_EXPERT * RECV, F), 1.0, 6.0, ((0, 32),))
    w_down = bell_draw(splits[1], (EXPERTS, F, D), F ** -0.5, 0.21875, ((0, 8), (1, 4)))
    expert_ids_keys = jax.random.split(jax.random.fold_in(splits[2], 1), TOKENS // TOK_DEV)
    expert_ids_turns = jax.random.permutation(jax.random.fold_in(splits[2], 3), TOKENS // TOK_DEV)
    expert_ids = jax.vmap(lambda own, number: assign_block(jax.random.fold_in(splits[2], 2), own, number, TOK_DEV, N_EXPERT, TOPK, CAP, 2))(expert_ids_keys, expert_ids_turns).reshape((TOKENS, TOPK))
    gates = jnp.clip(jnp.exp(math.log(1.0) - 2.9957323 * jax.random.uniform(splits[3], (TOKENS, TOPK), jnp.float32) ** level_of(splits[3], (TOKENS, TOPK), ((0, 32),), -0.2, 0.2)), 0.05, 1.0)
    cotangent = bell_draw(splits[4], (TOKENS, D), 1.0, 6.0, ((0, 32),))
    return {"hidden": hidden, "w_down": w_down, "expert_ids": expert_ids, "gates": gates, "cotangent": cotangent}


def positions(flat_ids):
    choose = (flat_ids[:, None] == jnp.arange(N_EXPERT, dtype=jnp.int32)[None, :]).astype(jnp.int32)
    earlier = jnp.cumsum(choose, axis=0) - choose
    return jnp.sum(earlier * choose, axis=1).astype(jnp.int32)


def reference(hidden, w_down, expert_ids, gates, cotangent):
    h_all = hidden.reshape(N_DP, N_EXPERT, N_EXPERT, CAP, F)
    id_all = expert_ids.reshape(N_DP, N_EXPERT, TOK_DEV, TOPK)
    gate_all = gates.reshape(N_DP, N_EXPERT, TOK_DEV, TOPK)
    cot_all = cotangent.reshape(N_DP, N_EXPERT, TOK_DEV, D)
    weight32 = w_down.astype(jnp.float32)
    senders = jnp.arange(N_EXPERT, dtype=jnp.int32)[:, None]
    highest = lax.Precision.HIGHEST

    def one_row(total, pieces):
        h_row, id_row, gate_row, cot_row = pieces
        h32 = h_row.astype(jnp.float32)
        outputs = jnp.einsum("ebcf,efd->ebcd", h32, weight32, precision=highest).astype(jnp.bfloat16)
        flat_ids = id_row.reshape(N_EXPERT, TOK_DEV * TOPK)
        position = jax.vmap(positions)(flat_ids)
        sender_ids = jnp.broadcast_to(senders, flat_ids.shape)
        picked = outputs[flat_ids, sender_ids, position].astype(jnp.float32).reshape(N_EXPERT, TOK_DEV, TOPK, D)
        cot32 = cot_row.astype(jnp.float32)
        mixed = jnp.sum(gate_row[..., None] * picked, axis=2).astype(jnp.bfloat16)
        gate_grads = jnp.sum(picked * cot32[:, :, None, :], axis=3)
        routed = (gate_row[..., None] * cot32[:, :, None, :]).astype(jnp.bfloat16).reshape(N_EXPERT, TOK_DEV * TOPK, D)
        grads_in = jnp.zeros((N_EXPERT, N_EXPERT, CAP, D), jnp.bfloat16).at[flat_ids, sender_ids, position].set(routed)
        grads32 = grads_in.astype(jnp.float32)
        hidden_grads = jnp.einsum("ebcd,efd->ebcf", grads32, weight32, precision=highest).astype(jnp.bfloat16)
        partial_sum = jnp.einsum("ebcf,ebcd->efd", h32, grads32, precision=highest).astype(jnp.bfloat16)
        partial_sum = lax.optimization_barrier(partial_sum)
        return total + partial_sum.astype(jnp.float32), (mixed, gate_grads, hidden_grads)

    start_total = jnp.zeros((N_EXPERT, F, D), jnp.float32)
    total, stacked = lax.scan(one_row, start_total, (h_all, id_all, gate_all, cot_all))
    mixed, gate_grads, hidden_grads = stacked
    return (mixed.reshape(N_DP * N_EXPERT * TOK_DEV, D), gate_grads.reshape(N_DP * N_EXPERT * TOK_DEV, TOPK), hidden_grads.reshape(N_DP * N_EXPERT * N_EXPERT * CAP, F), total.astype(jnp.bfloat16))
```

```python
import functools

import jax
import jax.numpy as jnp
from jax import lax
from jax.experimental import pallas as pl
from jax.experimental.pallas import tpu as pltpu
from jax.sharding import PartitionSpec as P

MESH = pl.DeviceIdType.MESH
F32 = jnp.float32
BF16 = jnp.bfloat16


VMEM_BYTES = 67043328


def kernel(
    nd, ne, C, S,
    hidden_in, w, ids, gates, cot,
    mixed, gate_grads, hidden_grads, weight_grads,
    hidden, wfull, cot_all, cot_far, meta, gg_send, gg_recv,
    ht, gh, ght, ght_far, z, wg_send1, wg_recv1, wg_send2, wg_recv2, wg_own, wg_hold,
    mx_send1, mx_recv1, mx_send2, mx_recv2, mx_own,
    wy_s, wy_r, wf_s, wf_r, zs, zr, xs, xr, cy_s, cy_r, hy_s, hy_r, gg_s, gg_r,
    g1_s, g1_r, g2_s, g2_r, m1_s, m1_r, m2_s, m2_r, lw, lc, lh,
):
    N = ne // 2
    rows, D = w.shape
    topk, tok = ids.shape
    F = hidden.shape[1]
    cap = hidden.shape[0] // ne
    T, cw = ne * tok, D // C
    summed = C - S
    a, e = lax.axis_index("dp"), lax.axis_index("expert")
    r, c = a // 2, a % 2
    q, x = e // 2, e % 2

    def to(a2, e2):
        return {"dp": a2, "expert": e2}

    pair_e, pair_c, pair_y = to(a, q * 2 + 1 - x), to(r * 2 + 1 - c, e), to((1 - r) * 2 + c, e)
    ahead, behind = to(a, ((q + 1) % N) * 2 + x), to(a, ((q + N - 1) % N) * 2 + x)
    not_last, not_first = q + 1 < N, q > 0
    onward = ((not_last, ahead), (not_first, behind))

    def copy_of(src, dst, ss, rs, dev):
        return pltpu.make_async_remote_copy(
            src_ref=src, dst_ref=dst, send_sem=ss, recv_sem=rs, device_id=dev, device_id_type=MESH
        )

    def remote(src, dst, ss, rs, dev):
        copy = copy_of(src, dst, ss, rs, dev)
        copy.start()
        return copy

    def w_rows(block):
        return pl.ds(pl.multiple_of(block * rows, rows), rows)

    def cols(j):
        return slice(j * cw, (j + 1) * cw)

    barrier = pltpu.get_barrier_semaphore()
    for dev in (pair_y, pair_c, pair_e):
        pl.semaphore_signal(barrier, inc=1, device_id=dev, device_id_type=MESH)
    for exists, dev in onward:

        @pl.when(exists)
        def _():
            pl.semaphore_signal(barrier, inc=1, device_id=dev, device_id_type=MESH)

    own_w, own_c = [], []
    for j in range(C):
        own_w.append(pltpu.make_async_copy(w.at[:, cols(j)], wfull.at[j, w_rows(a)], lw.at[j]))
        own_c.append(pltpu.make_async_copy(cot.at[:, cols(j)], cot_all.at[j, q, x], lc.at[j]))
        own_w[j].start()
        own_c[j].start()
    own_h = pltpu.make_async_copy(hidden_in, hidden, lh.at[0])
    own_h.start()

    meta[q, x] = jnp.zeros(meta.shape[2:], F32)
    idf = ids[...].astype(F32)
    meta[q, x, 0:topk, 0:tok] = idf
    meta[q, x, topk : 2 * topk, 0:tok] = gates[...]
    gg_send[...] = jnp.zeros_like(gg_send)

    for j in range(C):
        own_w[j].wait()
        own_c[j].wait()

    pl.semaphore_wait(barrier, 3 + not_last.astype(jnp.int32) + not_first.astype(jnp.int32))

    def block(i, zq, xq):
        if i == 0:
            return meta.at[zq, xq]
        if i <= C:
            return cot_all.at[i - 1, zq, xq]
        return cot_far.at[i - 1 - C, zq, xq]

    def line(i, side, d):
        ref = block(i, q + d if side else q - d, x)
        return copy_of(ref, ref, zs.at[i, side, d], zr.at[i, side, d], onward[side][1])

    def arrival(i, side, d):
        ref = block(i, q + d if side else q - d, x)
        return copy_of(ref, ref, zs.at[i, side, d - 1], zr.at[i, side, d - 1], onward[side][1])

    def across(i, zq, xq):
        ref = block(i, zq, xq)
        return copy_of(ref, ref, xs.at[i, zq], xr.at[i, zq], pair_e)

    def there(side, d):
        return q + d < N if side else q >= d

    def begin(i):
        for side in range(2):

            @pl.when(onward[side][0])
            def _():
                line(i, side, 0).start()

        across(i, q, x).start()

    def step(i, d):
        for side in range(2):

            @pl.when(there(side, d))
            def _():
                arrival(i, side, d).wait_recv()
                if d < N - 1:

                    @pl.when(onward[side][0])
                    def _():
                        line(i, side, d).start()

                across(i, q + d if side else q - d, x).start()

    complete = set()

    def gathered(i):
        if i not in complete:
            complete.add(i)
            for zq in range(N):
                across(i, zq, 1 - x).wait_recv()

    def sent(i):
        for side in range(2):
            for d in range(N - 1):

                @pl.when(onward[side][0] & there(side, d))
                def _():
                    line(i, side, d).wait_send()

        for zq in range(N):
            across(i, zq, x).wait_send()

    wy, wf, cy, g1, g2, m1, m2, gg, hy = ({} for _ in range(9))
    order = sorted(range(1, N), key=lambda d: min(d, N - d))

    begin(0)

    def send_w(j):
        mine = wfull.at[j, w_rows(a)]
        wy[j] = remote(mine, mine, wy_s.at[j], wy_r.at[j], pair_y)

    def send_far(s):
        cy[s] = remote(
            cot_all.at[summed + s, q, x], cot_far.at[s, q, x], cy_s.at[s], cy_r.at[s], pair_y
        )

    for j in range(C):
        send_w(j)
        if j == C // 2 - 1:
            for s in range(S):
                send_far(s)
        begin(1 + j)
    for j in range(C):
        mine = wfull.at[j, w_rows(a)]
        wf[0, j] = remote(mine, mine, wf_s.at[0, j], wf_r.at[0, j], pair_c)

    def forward_w(j):
        theirs = wfull.at[j, w_rows((1 - r) * 2 + c)]
        wy[j].wait_recv()
        wf[1, j] = remote(theirs, theirs, wf_s.at[1, j], wf_r.at[1, j], pair_c)

    def placer(slot_row):
        return (lax.broadcasted_iota(jnp.int32, (cap, tok), 0).astype(F32) == slot_row).astype(BF16)

    eye = lax.broadcasted_iota(jnp.int32, (tok, tok), 0) == lax.broadcasted_iota(jnp.int32, (tok, tok), 1)

    def to_row(col):
        return jnp.sum(jnp.where(eye, col, 0.0), axis=0, keepdims=True)

    def to_col(row):
        return jnp.sum(jnp.where(eye, row, 0.0), axis=1, keepdims=True)

    def routes():
        upper = (
            lax.broadcasted_iota(jnp.int32, (tok, tok), 0) < lax.broadcasted_iota(jnp.int32, (tok, tok), 1)
        ).astype(BF16)
        chosen, weight = [], []
        for b in range(ne):
            tile = meta[b // 2, b % 2]
            hit = tile[0:topk, 0:tok] == e.astype(F32)
            chosen.append(jnp.sum(jnp.where(hit, 1.0, 0.0), axis=0, keepdims=True))
            weight.append(jnp.sum(jnp.where(hit, tile[topk : 2 * topk, 0:tok], 0.0), axis=0, keepdims=True))
        choose = jnp.concatenate(chosen, axis=0)
        position = jnp.dot(choose.astype(BF16), upper, preferred_element_type=F32)
        slots = jnp.where(choose > 0.0, position, -1.0)
        return [slots[b : b + 1, :] for b in range(ne)], weight

    def pick(slot_rows, gate_rows):
        for b in range(ne):
            rows_b = lax.dot_general(
                placer(slot_rows[b]), hidden[b * cap : (b + 1) * cap, :], (((0,), (0,)), ((), ())),
                preferred_element_type=F32,
            )
            ht[b // 2, b % 2] = rows_b.astype(BF16)
            gh[b // 2, b % 2] = (to_col(gate_rows[b]) * rows_b).astype(BF16)
        ght[...] = gh[...].reshape(T, F).astype(F32).T.astype(BF16)

    def begin_grads(j):
        gathered(1 + j)
        right = cot_all[j].reshape(T, cw)

        def block_of(b):
            return jnp.dot(ght[w_rows(b), :], right, preferred_element_type=F32)

        if j < summed:
            for k in range(2):
                wg_send1[j, k] = block_of(((r + k) % 2) * 2 + 1 - c).astype(BF16)
            g1[j] = remote(wg_send1.at[j], wg_recv1.at[j], g1_s.at[j], g1_r.at[j], pair_c)
            wg_hold[j] = block_of((1 - r) * 2 + c)
            wg_own[j] = block_of(r * 2 + c)
            return
        s = j - summed
        gathered(1 + C + s)
        if s == 0:
            hy[0].wait_recv()
        far = cot_far[s].reshape(T, cw)

        def both(core):
            other = jnp.dot(ght_far[w_rows(core), :], far, preferred_element_type=F32)
            return block_of(r * 2 + core) + other

        wg_send1[j, 0] = both(1 - c).astype(BF16)
        g1[j] = remote(wg_send1.at[j, 0], wg_recv1.at[j, 0], g1_s.at[j], g1_r.at[j], pair_c)
        wg_own[j] = both(c)

    def pass_grads(j):
        g1[j].wait_recv()
        wg_send2[j] = (wg_hold[j] + wg_recv1[j, 1].astype(F32)).astype(BF16)
        g2[j] = remote(wg_send2.at[j], wg_recv2.at[j], g2_s.at[j], g2_r.at[j], pair_y)

    def out_part(j):
        for d in range(2):
            wf[d, j].wait_recv()
        left = gh[:, pl.ds(1 - x, 1)].reshape(N * tok, F)
        val = jnp.dot(left, wfull[j], preferred_element_type=F32)
        mx_send1[j] = val.astype(BF16).reshape(N, tok, cw)
        m1[j] = remote(mx_send1.at[j], mx_recv1.at[j], m1_s.at[j], m1_r.at[j], pair_e)
        left = gh[:, pl.ds(x, 1)].reshape(N * tok, F)
        val = jnp.dot(left, wfull[j], preferred_element_type=F32)
        mx_own[j] = val.reshape(N, tok, cw)

    def z_part(j):
        gathered(1 + j)
        val = lax.dot_general(
            cot_all[j].reshape(T, cw), wfull[j], (((1,), (1,)), ((), ())), preferred_element_type=F32
        )
        z[...] = val if j == 0 else z[...] + val

    def mix_part(j):
        m1[j].wait_recv()
        for k in order:
            o = (q + k) % N
            mx_send2[j, o] = (mx_own[j, o] + mx_recv1[j, o].astype(F32)).astype(BF16)
            m2[k, j] = remote(
                mx_send2.at[j, o], mx_recv2.at[j, q], m2_s.at[k - 1, j], m2_r.at[k - 1, j],
                to(a, o * 2 + x),
            )

    def hidden_part(slot_rows, gate_rows):
        for b in range(ne):
            zb = z[b * tok : (b + 1) * tok, :]
            gg_col = jnp.sum(ht[b // 2, b % 2].astype(F32) * zb, axis=1, keepdims=True)
            gg_send[b // 2, b % 2, 0:1, 0:tok] = to_row(gg_col)
            scaled = (to_col(gate_rows[b]) * zb).astype(BF16)
            hidden_grads[b * cap : (b + 1) * cap, :] = jnp.dot(
                placer(slot_rows[b]), scaled, preferred_element_type=F32
            ).astype(BF16)
        for d in range(1, ne):
            o = (e + d) % ne
            gg[d] = remote(
                gg_send.at[o // 2, o % 2], gg_recv.at[q, x], gg_s.at[d - 1], gg_r.at[d - 1], to(a, o)
            )
        gg_recv[q, x] = gg_send[q, x]

    far_items = [1 + C + s for s in range(S)]
    half = C // 2
    for i in range(C + 1):
        step(i, 1)
    for i in range(half + 1):
        step(i, 2)
    forward_w(0)
    for i in range(half + 1, C + 1):
        step(i, 2)
    for i in range(half + 1):
        for d in range(3, N):
            step(i, d)
    own_h.wait()
    gathered(0)
    slot_rows, gate_rows = routes()
    pick(slot_rows, gate_rows)
    if S:
        there_rows = pl.ds(pl.multiple_of((1 - r) * 2 * rows, 2 * rows), 2 * rows)
        hy[0] = remote(ght.at[there_rows], ght_far, hy_s.at[0], hy_r.at[0], pair_y)
    out_part(0)
    forward_w(1)
    for i in range(half + 1, C + 1):
        for d in range(3, N):
            step(i, d)
    begin_grads(0)
    out_part(1)
    for s in range(S):
        cy[s].wait_recv()
        begin(far_items[s])
    z_part(0)
    pass_grads(0)
    begin_grads(1)
    z_part(1)
    for i in far_items:
        step(i, 1)
    mix_part(0)
    pass_grads(1)
    for d in range(2, N):
        for i in far_items:
            step(i, d)
    forward_w(2)
    out_part(2)
    mix_part(1)
    if summed > 2:
        begin_grads(2)
    z_part(2)
    if summed > 2:
        pass_grads(2)
    forward_w(3)
    out_part(3)
    mix_part(2)
    if summed > 3:
        begin_grads(3)
    z_part(3)
    if summed > 3:
        pass_grads(3)
    hidden_part(slot_rows, gate_rows)
    mix_part(3)
    for j in range(summed, C):
        begin_grads(j)

    for j in range(C):
        total = mx_own[j, q] + mx_recv1[j, q].astype(F32)
        for k in order:
            m2[k, j].wait_recv()
            total = total + mx_recv2[j, (q - k + N) % N].astype(F32)
        mixed[:, cols(j)] = total.astype(BF16)

    for d in range(1, ne):
        gg[d].wait_recv()
    for k in range(topk):
        row = jnp.zeros((1, tok), F32)
        for b in range(ne):
            row = row + jnp.where(idf[k : k + 1, :] == float(b), gg_recv[b // 2, b % 2, 0:1, 0:tok], 0.0)
        gate_grads[k : k + 1, :] = row

    for j in range(summed, C):
        g1[j].wait_recv()
        weight_grads[:, cols(j)] = (wg_own[j] + wg_recv1[j, 0].astype(F32)).astype(BF16)
    for j in range(summed):
        val = wg_own[j] + wg_recv1[j, 0].astype(F32)
        g2[j].wait_recv()
        weight_grads[:, cols(j)] = (val + wg_recv2[j].astype(F32)).astype(BF16)

    for group in (wy, wf, cy, g1, g2, m1, m2, gg, hy):
        for copy in group.values():
            copy.wait_send()
    for i in range(1 + C + S):
        sent(i)


def store_kernel(count, *refs):
    sems = refs[-1]
    copies = [pltpu.make_async_copy(refs[i], refs[count + i], sems.at[i]) for i in range(count)]
    for copy in copies:
        copy.start()
    for copy in copies:
        copy.wait()


def fused(hidden, weight_rows, expert_ids, gates, cotangent):
    nd, ne = lax.axis_size("dp"), lax.axis_size("expert")
    rows, D = weight_rows.shape
    tok, topk = expert_ids.shape
    F = hidden.shape[1]
    T, N = ne * tok, ne // 2
    C, S = 4, 2
    cw, items, summed = D // C, 1 + C + S, C - S
    vm = pltpu.VMEM
    sem = lambda *n: pltpu.SemaphoreType.DMA(tuple(max(i, 1) for i in n))
    near, far = pl.BlockSpec(memory_space=pltpu.VMEM), pl.BlockSpec(memory_space=pltpu.HBM)
    shapes = [((tok, D), BF16), ((topk, tok), F32), (hidden.shape, BF16), ((rows, D), BF16)]
    few, some = max(S, 1), max(summed, 1)
    tall = -(-2 * topk // 8) * 8
    result_bytes = 2 * (tok * D + hidden.size + rows * D) + 128 * 1024
    results = pl.pallas_call(
        functools.partial(kernel, nd, ne, C, S),
        out_shape=tuple(pltpu.VMEM(*s) for s in shapes),
        in_specs=[far, far, near, near, far],
        out_specs=(near,) * 4,
        scratch_shapes=[
            vm(hidden.shape, BF16), vm((C, F, cw), BF16), vm((C, N, 2, tok, cw), BF16),
            vm((few, N, 2, tok, cw), BF16), vm((N, 2, tall, 128), F32),
            vm((N, 2, 8, 128), F32), vm((N, 2, 8, 128), F32),
            vm((N, 2, tok, F), BF16), vm((N, 2, tok, F), BF16), vm((F, T), BF16), vm((2 * rows, T), BF16),
            vm((T, F), F32),
            vm((C, 2, rows, cw), BF16), vm((C, 2, rows, cw), BF16),
            vm((some, rows, cw), BF16), vm((some, rows, cw), BF16), vm((C, rows, cw), F32),
            vm((some, rows, cw), F32),
            vm((C, N, tok, cw), BF16), vm((C, N, tok, cw), BF16),
            vm((C, N, tok, cw), BF16), vm((C, N, tok, cw), BF16), vm((C, N, tok, cw), F32),
            sem(C), sem(C), sem(2, C), sem(2, C),
            sem(items, 2, N - 1), sem(items, 2, N - 1), sem(items, N), sem(items, N),
            sem(S), sem(S), sem(1), sem(1), sem(ne - 1), sem(ne - 1),
            sem(C), sem(C), sem(summed), sem(summed),
            sem(C), sem(C), sem(N - 1, C), sem(N - 1, C), sem(C), sem(C), sem(1),
        ],
        compiler_params=pltpu.CompilerParams(
            collective_id=0, has_side_effects=True, vmem_limit_bytes=VMEM_BYTES - result_bytes
        ),
    )(hidden, weight_rows, expert_ids.T, gates.T, cotangent)
    mixed, gate_grads, hidden_grads, sums = pl.pallas_call(
        functools.partial(store_kernel, len(shapes)),
        out_shape=tuple(jax.ShapeDtypeStruct(*s) for s in shapes),
        in_specs=[pl.BlockSpec(memory_space=pl.ANY)] * 4,
        out_specs=(far,) * 4,
        scratch_shapes=[sem(len(shapes))],
        compiler_params=pltpu.CompilerParams(vmem_limit_bytes=1024 * 1024),
    )(*results)
    return mixed, gate_grads.T, hidden_grads, sums


def slot_table(expert_ids, experts, capacity):
    flat_ids = expert_ids.reshape(-1)
    choose = (flat_ids[:, None] == jnp.arange(experts, dtype=jnp.int32)[None, :]).astype(jnp.int32)
    earlier = jnp.cumsum(choose, axis=0) - choose
    position = jnp.sum(earlier * choose, axis=1)
    target = flat_ids * capacity + position
    return (target[None, :] == jnp.arange(experts * capacity, dtype=jnp.int32)[:, None]).astype(BF16)


def plain(hidden, weight_rows, expert_ids, gates, cotangent):
    experts = lax.axis_size("expert")
    capacity = hidden.shape[0] // experts
    tok, topk = expert_ids.shape
    width = cotangent.shape[1]
    table = slot_table(expert_ids, experts, capacity)
    weight = lax.all_gather(weight_rows, "dp", axis=0, tiled=True)
    outputs = jnp.dot(hidden, weight, preferred_element_type=F32).astype(BF16)
    back = lax.all_to_all(outputs, "expert", split_axis=0, concat_axis=0, tiled=True)
    picked = lax.dot_general(table, back, (((0,), (0,)), ((), ())), preferred_element_type=F32)
    picked = picked.reshape(tok, topk, width)
    cot32 = cotangent.astype(F32)[:, None, :]
    mixed = jnp.sum(gates[:, :, None] * picked, axis=1).astype(BF16)
    gate_grads = jnp.sum(picked * cot32, axis=2)
    routed = (gates[:, :, None] * cot32).astype(BF16).reshape(-1, width)
    packed = jnp.dot(table, routed, preferred_element_type=F32).astype(BF16)
    grads = lax.all_to_all(packed, "expert", split_axis=0, concat_axis=0, tiled=True)
    hidden_grads = lax.dot_general(
        grads, weight, (((1,), (1,)), ((), ())), preferred_element_type=F32
    ).astype(BF16)
    partial = lax.dot_general(
        hidden, grads, (((0,), (0,)), ((), ())), preferred_element_type=F32
    ).astype(BF16)
    sums = lax.psum_scatter(partial, "dp", scatter_dimension=0, tiled=True)
    return mixed, gate_grads, hidden_grads, sums


def per_device(hidden, w_down, expert_ids, gates, cotangent):
    nd, ne = lax.axis_size("dp"), lax.axis_size("expert")
    rows, width = w_down.shape[1:]
    cap, tok = hidden.shape[0] // ne, expert_ids.shape[0]
    tiled = rows % 16 == 0 and cap % 16 == 0 and tok % 16 == 0 and tok <= 128
    paired = nd == 4 and ne % 2 == 0 and width % 512 == 0
    small = expert_ids.shape[1] <= 8
    body = fused if tiled and paired and small else plain
    mixed, gate_grads, hidden_grads, sums = body(
        hidden, w_down.reshape(rows, width), expert_ids, gates, cotangent
    )
    return mixed, gate_grads, hidden_grads, sums.reshape(1, rows, width)


def solution(mesh):
    split = P(("dp", "expert"), None)
    weights = P("expert", "dp", None)
    return jax.shard_map(
        per_device,
        mesh=mesh,
        in_specs=(split, weights, split, split, split),
        out_specs=(split, split, split, weights),
        check_vma=False,
    )
```

```python
import functools

import jax
import jax.numpy as jnp
from jax import lax
from jax.experimental import pallas as pl
from jax.experimental.pallas import tpu as pltpu
from jax.sharding import PartitionSpec as P

MESH = pl.DeviceIdType.MESH
F32 = jnp.float32
BF16 = jnp.bfloat16


VMEM_BYTES = 67043328


def kernel(
    nd, ne, C, S, K,
    hidden_in, w, ids, gates, cot,
    mixed, gate_grads, hidden_grads, weight_grads,
    hidden, wfull, cot_all, cot_far, meta, gg_send, gg_recv,
    ht, gh, ght, ght_far, z, wg_send1, wg_recv1, wg_part, wg_recvp, wg_send2, wg_recv2, wg_own, wg_hold,
    mx_send1, mx_recv1, mx_send2, mx_recv2, mx_own,
    wy_s, wy_r, wf_s, wf_r, zs, zr, xs, xr, zms, zmr, xms, xmr, zfs, zfr, xfs, xfr, cy_s, cy_r, hy_s, hy_r, gg_s, gg_r,
    g1_s, g1_r, g2_s, g2_r, m1_s, m1_r, m2_s, m2_r, local,
):
    N = ne // 2
    rows, D = w.shape
    topk, tok = ids.shape
    F = hidden.shape[1]
    cap = hidden.shape[0] // ne
    T, cw, vw = ne * tok, D // C, D // K
    summed = C - S
    a, e = lax.axis_index("dp"), lax.axis_index("expert")
    r, c = a // 2, a % 2
    q, x = e // 2, e % 2

    def to(a2, e2):
        return {"dp": a2, "expert": e2}

    pair_e, pair_c, pair_y = to(a, q * 2 + 1 - x), to(r * 2 + 1 - c, e), to((1 - r) * 2 + c, e)
    ahead, behind = to(a, ((q + 1) % N) * 2 + x), to(a, ((q + N - 1) % N) * 2 + x)
    not_last, not_first = q + 1 < N, q > 0
    onward = ((not_last, ahead), (not_first, behind))

    def copy_of(src, dst, ss, rs, dev):
        return pltpu.make_async_remote_copy(
            src_ref=src, dst_ref=dst, send_sem=ss, recv_sem=rs, device_id=dev, device_id_type=MESH
        )

    def start(src, dst, ss, rs, dev):
        copy_of(src, dst, ss, rs, dev).start()

    def arrived(ref, sem):
        copy_of(ref, ref, sem, sem, pair_e).wait_recv()

    def left(ref, sem):
        copy_of(ref, ref, sem, sem, pair_e).wait_send()

    def w_rows(block):
        return pl.ds(pl.multiple_of(block * rows, rows), rows)

    def cols(j, width=cw):
        return slice(j * width, (j + 1) * width)

    barrier = pltpu.get_barrier_semaphore()
    for dev in (pair_y, pair_c, pair_e):
        pl.semaphore_signal(barrier, inc=1, device_id=dev, device_id_type=MESH)
    for exists, dev in onward:

        @pl.when(exists)
        def _():
            pl.semaphore_signal(barrier, inc=1, device_id=dev, device_id_type=MESH)

    for j in range(K):
        pltpu.make_async_copy(w.at[:, cols(j, vw)], wfull.at[j, w_rows(a)], local.at[0]).start()
    for j in range(C):
        pltpu.make_async_copy(cot.at[:, cols(j)], cot_all.at[j, q, x], local.at[1]).start()
    own_h = pltpu.make_async_copy(hidden_in, hidden, local.at[2])
    own_h.start()

    meta[q, x] = jnp.zeros(meta.shape[2:], F32)
    idf = ids[...].astype(F32)
    meta[q, x, 0:topk, 0:tok] = idf
    meta[q, x, topk : 2 * topk, 0:tok] = gates[...]
    gg_send[...] = jnp.zeros_like(gg_send)

    mine, theirs = w_rows(a), w_rows((1 - r) * 2 + c)
    pltpu.make_async_copy(wfull.at[:, mine], wfull.at[:, mine], local.at[0]).wait()
    own_c = cot_all.at[:, q, x]
    pltpu.make_async_copy(own_c, own_c, local.at[1]).wait()
    pl.semaphore_wait(barrier, 3 + not_last.astype(jnp.int32) + not_first.astype(jnp.int32))

    def there(side, d):
        return q + d < N if side else q >= d

    def at(side, d):
        return q + d if side else q - d

    def pair_of(p, zq):
        return meta.at[zq] if p < 0 else cot_far.at[p, zq]

    def pass_pair(p, side, d):
        zq = at(side, d)
        ref = pair_of(p, zq)
        if p < 0:
            start(ref, ref, zms.at[side, d], zmr.at[zq], onward[side][1])
        else:
            start(ref, ref, zfs.at[side, d], zfr.at[p, zq], onward[side][1])

    def pass_cot(i, side, d):
        ref = cot_all.at[i, at(side, d), x]
        start(ref, ref, zs.at[side, d], zr.at[i, at(side, d)], onward[side][1])

    def across(i, zq):
        ref = cot_all.at[i, zq, x]
        start(ref, ref, xs.at[0], xr.at[i], pair_e)

    def pair_cross(p):
        ref = pair_of(p, q).at[x]
        if p < 0:
            start(ref, ref, xms.at[0], xmr.at[0], pair_e)
        else:
            start(ref, ref, xfs.at[0], xfr.at[p], pair_e)

    def pair_step(p, d):
        if d == 0:
            arrived(pair_of(p, q).at[1 - x], xmr.at[0] if p < 0 else xfr.at[p])
        for side in range(2):

            @pl.when(there(side, d) if d else onward[side][0])
            def _():
                if d:
                    arrived(pair_of(p, at(side, d)), zmr.at[at(side, d)] if p < 0 else zfr.at[p, at(side, d)])
                if 0 < d < N - 1:

                    @pl.when(onward[side][0])
                    def _():
                        pass_pair(p, side, d)

                if d == 0:
                    pass_pair(p, side, d)

    def begin(i):
        for side in range(2):

            @pl.when(onward[side][0])
            def _():
                pass_cot(i, side, 0)

    def step(i, d):
        for side in range(2):

            @pl.when(there(side, d))
            def _():
                arrived(cot_all.at[i, at(side, d), x], zr.at[i, at(side, d)])
                if d < N - 1:

                    @pl.when(onward[side][0])
                    def _():
                        pass_cot(i, side, d)

                across(i, at(side, d))

    def begin_far():
        arrived(cot_far.at[:, q, x], cy_r.at[0])
        for s in range(S):
            pair_cross(s)

    complete = set()

    def gathered(i):
        if i not in complete:
            complete.add(i)
            arrived(cot_all.at[i, :, 1 - x], xr.at[i])

    order = sorted(range(1, N), key=lambda d: min(d, N - d))

    def send_w(j):
        ref = wfull.at[j, mine]
        start(ref, ref, wy_s.at[0], wy_r.at[j], pair_y)

    def share_w(j):
        ref = wfull.at[j, mine]
        start(ref, ref, wf_s.at[0], wf_r.at[j], pair_c)

    def forward_w(j):
        ref = wfull.at[j, theirs]
        arrived(ref, wy_r.at[j])
        start(ref, ref, wf_s.at[0], wf_r.at[j], pair_c)

    def send_far():
        start(
            cot_all.at[summed:C, q, x], cot_far.at[:, q, x], cy_s.at[0], cy_r.at[0], pair_y
        )

    def placer(slot_row):
        return (lax.broadcasted_iota(jnp.int32, (cap, tok), 0).astype(F32) == slot_row).astype(BF16)

    eye = lax.broadcasted_iota(jnp.int32, (tok, tok), 0) == lax.broadcasted_iota(jnp.int32, (tok, tok), 1)

    def to_row(col):
        return jnp.sum(jnp.where(eye, col, 0.0), axis=0, keepdims=True)

    def to_col(row):
        return jnp.sum(jnp.where(eye, row, 0.0), axis=1, keepdims=True)

    def routes():
        upper = (
            lax.broadcasted_iota(jnp.int32, (tok, tok), 0) < lax.broadcasted_iota(jnp.int32, (tok, tok), 1)
        ).astype(BF16)
        chosen, weight = [], []
        for b in range(ne):
            tile = meta[b // 2, b % 2]
            hit = tile[0:topk, 0:tok] == e.astype(F32)
            chosen.append(jnp.sum(jnp.where(hit, 1.0, 0.0), axis=0, keepdims=True))
            weight.append(jnp.sum(jnp.where(hit, tile[topk : 2 * topk, 0:tok], 0.0), axis=0, keepdims=True))
        choose = jnp.concatenate(chosen, axis=0)
        position = jnp.dot(choose.astype(BF16), upper, preferred_element_type=F32)
        slots = jnp.where(choose > 0.0, position, -1.0)
        return [slots[b : b + 1, :] for b in range(ne)], weight

    def pick(slot_rows, gate_rows):
        for b in range(ne):
            rows_b = lax.dot_general(
                placer(slot_rows[b]), hidden[b * cap : (b + 1) * cap, :], (((0,), (0,)), ((), ())),
                preferred_element_type=F32,
            )
            ht[b // 2, b % 2] = rows_b.astype(BF16)
            gh[b // 2, b % 2] = (to_col(gate_rows[b]) * rows_b).astype(BF16)
        ght[...] = gh[...].reshape(T, F).astype(F32).T.astype(BF16)

    def send_rows():
        there_rows = pl.ds(pl.multiple_of((1 - r) * 2 * rows, 2 * rows), 2 * rows)
        start(ght.at[there_rows], ght_far, hy_s.at[0], hy_r.at[0], pair_y)

    def block_of(j, b):
        return jnp.dot(ght[w_rows(b), :], cot_all[j].reshape(T, cw), preferred_element_type=F32)

    def begin_grads(j):
        gathered(j)
        for k in range(2):
            wg_send1[j, k] = block_of(j, ((r + k) % 2) * 2 + 1 - c).astype(BF16)
        start(wg_send1.at[j], wg_recv1.at[j], g1_s.at[0], g1_r.at[j], pair_c)
        wg_hold[j] = block_of(j, (1 - r) * 2 + c)
        wg_own[j] = block_of(j, r * 2 + c)

    def pass_grads(j):
        arrived(wg_recv1.at[j], g1_r.at[j])
        wg_send2[j] = (wg_hold[j] + wg_recv1[j, 1].astype(F32)).astype(BF16)
        start(wg_send2.at[j], wg_recv2.at[j], g2_s.at[0], g2_r.at[j], pair_y)

    def full_grads(j):
        s = j - summed
        gathered(j)
        if s == 0:
            arrived(ght_far, hy_r.at[0])

        def both(core):
            other = jnp.dot(
                ght_far[w_rows(core), :], cot_far[s].reshape(T, cw), preferred_element_type=F32
            )
            return block_of(j, r * 2 + core) + other

        wg_part[s] = both(1 - c).astype(BF16)
        start(wg_part.at[s], wg_recvp.at[s], g1_s.at[1], g1_r.at[j], pair_c)
        wg_own[j] = both(c)

    def out_part(j):
        arrived(wfull.at[j, 0 : 2 * rows], wf_r.at[j])
        lhs = gh[:, pl.ds(1 - x, 1)].reshape(N * tok, F)
        val = jnp.dot(lhs, wfull[j], preferred_element_type=F32)
        mx_send1[j] = val.astype(BF16).reshape(N, tok, vw)
        start(mx_send1.at[j], mx_recv1.at[j], m1_s.at[0], m1_r.at[j], pair_e)
        lhs = gh[:, pl.ds(x, 1)].reshape(N * tok, F)
        val = jnp.dot(lhs, wfull[j], preferred_element_type=F32)
        mx_own[j] = val.reshape(N, tok, vw)

    def z_part(j):
        i = j * vw // cw
        gathered(i)
        part = cot_all[i, :, :, :, cols(j % (cw // vw), vw)].reshape(T, vw)
        val = lax.dot_general(part, wfull[j], (((1,), (1,)), ((), ())), preferred_element_type=F32)
        z[...] = val if j == 0 else z[...] + val

    def mix_part(j):
        arrived(mx_recv1.at[j], m1_r.at[j])
        for k in order:
            o = (q + k) % N
            mx_send2[j, o] = (mx_own[j, o] + mx_recv1[j, o].astype(F32)).astype(BF16)
            start(mx_send2.at[j, o], mx_recv2.at[j, q], m2_s.at[0], m2_r.at[j], to(a, o * 2 + x))

    def hidden_part(slot_rows, gate_rows):
        for b in range(ne):
            zb = z[b * tok : (b + 1) * tok, :]
            gg_col = jnp.sum(ht[b // 2, b % 2].astype(F32) * zb, axis=1, keepdims=True)
            gg_send[b, 0:1, 0:tok] = to_row(gg_col)
            scaled = (to_col(gate_rows[b]) * zb).astype(BF16)
            hidden_grads[b * cap : (b + 1) * cap, :] = jnp.dot(
                placer(slot_rows[b]), scaled, preferred_element_type=F32
            ).astype(BF16)
        for d in range(1, ne):
            o = (e + d) % ne
            start(gg_send.at[o], gg_recv.at[e], gg_s.at[0], gg_r.at[0], to(a, o))
        gg_recv[e] = gg_send[e]

    def finish_mixed(j):
        arrived(mx_recv2.at[j, 0 : N - 1], m2_r.at[j])
        total = mx_own[j, q] + mx_recv1[j, q].astype(F32)
        for k in order:
            total = total + mx_recv2[j, (q - k + N) % N].astype(F32)
        mixed[:, cols(j, vw)] = total.astype(BF16)

    def finish_gates():
        arrived(gg_recv.at[0 : ne - 1], gg_r.at[0])
        for k in range(topk):
            row = jnp.zeros((1, tok), F32)
            for b in range(ne):
                row = row + jnp.where(idf[k : k + 1, :] == float(b), gg_recv[b, 0:1, 0:tok], 0.0)
            gate_grads[k : k + 1, :] = row

    def finish_grads(j):
        if j >= summed:
            arrived(wg_recvp.at[j - summed], g1_r.at[j])
            weight_grads[:, cols(j)] = (wg_own[j] + wg_recvp[j - summed].astype(F32)).astype(BF16)
            return
        val = wg_own[j] + wg_recv1[j, 0].astype(F32)
        arrived(wg_recv2.at[j], g2_r.at[j])
        weight_grads[:, cols(j)] = (val + wg_recv2[j].astype(F32)).astype(BF16)

    pair_cross(-1)
    send_far()
    for j in range(K):
        send_w(j)
    for j in range(C):
        across(j, q)
    begin(0)
    begin(1)
    for j in range(K):
        share_w(j)
    pair_step(-1, 0)
    begin(2)
    begin(3)
    begin_far()
    step(0, 1)
    step(1, 1)
    pair_step(-1, 1)
    step(2, 1)
    step(3, 1)
    step(0, 2)
    step(1, 2)
    pair_step(-1, 2)
    forward_w(0)
    pair_step(0, 0)
    step(2, 2)
    step(3, 2)
    pair_step(1, 0)
    step(0, 3)
    step(1, 3)
    pair_step(-1, 3)
    own_h.wait()
    slot_rows, gate_rows = routes()
    pick(slot_rows, gate_rows)
    forward_w(1)
    out_part(0)
    send_rows()
    forward_w(2)
    step(2, 3)
    step(3, 3)
    forward_w(3)
    out_part(1)
    forward_w(4)
    out_part(2)
    out_part(3)
    mix_part(0)
    forward_w(5)
    pair_step(0, 1)
    out_part(4)
    pair_step(1, 1)
    z_part(0)
    z_part(1)
    forward_w(6)
    mix_part(1)
    out_part(5)
    begin_grads(0)
    forward_w(7)
    mix_part(2)
    pair_step(0, 2)
    out_part(6)
    mix_part(3)
    pair_step(1, 2)
    pass_grads(0)
    out_part(7)
    mix_part(4)
    z_part(2)
    z_part(3)
    z_part(4)
    mix_part(5)
    z_part(5)
    z_part(6)
    z_part(7)
    mix_part(6)
    hidden_part(slot_rows, gate_rows)
    begin_grads(1)
    mix_part(7)
    pass_grads(1)
    pair_step(0, 3)
    full_grads(2)
    pair_step(1, 3)
    full_grads(3)
    for j in range(K - 2):
        finish_mixed(j)
    finish_gates()
    finish_grads(2)
    finish_mixed(K - 2)
    finish_mixed(K - 1)
    finish_grads(0)
    finish_grads(3)
    finish_grads(1)

    left(wfull.at[:, mine], wy_s.at[0])
    left(wfull.at[:, 0 : 2 * rows], wf_s.at[0])
    left(cot_far.at[:, 0, 0], cy_s.at[0])
    left(cot_all.at[:, :, 0], xs.at[0])
    left(cot_far.at[:, 0, 0], xfs.at[0])
    left(meta.at[0, 0], xms.at[0])
    left(ght_far, hy_s.at[0])
    for side in range(2):
        for d in range(N - 1):

            @pl.when(onward[side][0] & there(side, d))
            def _():
                left(meta.at[0], zms.at[side, d])
                left(cot_all.at[:, 0, 0], zs.at[side, d])
                left(cot_far.at[:, 0], zfs.at[side, d])

    left(wg_send1, g1_s.at[0])
    left(wg_part, g1_s.at[1])
    left(mx_send1, m1_s.at[0])
    left(gg_send.at[0 : ne - 1], gg_s.at[0])
    left(mx_send2.at[:, 0 : N - 1], m2_s.at[0])
    left(wg_send2, g2_s.at[0])


def store_kernel(count, *refs):
    sems = refs[-1]
    copies = [pltpu.make_async_copy(refs[i], refs[count + i], sems.at[i]) for i in range(count)]
    for copy in copies:
        copy.start()
    for copy in copies:
        copy.wait()


def fused(hidden, weight_rows, expert_ids, gates, cotangent):
    nd, ne = lax.axis_size("dp"), lax.axis_size("expert")
    rows, D = weight_rows.shape
    tok, topk = expert_ids.shape
    F = hidden.shape[1]
    T, N = ne * tok, ne // 2
    C, S, K = 4, 2, 8
    cw, vw, summed = D // C, D // K, C - S
    vm = pltpu.VMEM
    sem = lambda *n: pltpu.SemaphoreType.DMA(tuple(max(i, 1) for i in n))
    near, far = pl.BlockSpec(memory_space=pltpu.VMEM), pl.BlockSpec(memory_space=pltpu.HBM)
    shapes = [((tok, D), BF16), ((topk, tok), F32), (hidden.shape, BF16), ((rows, D), BF16)]
    tall = -(-2 * topk // 8) * 8
    result_bytes = 2 * (tok * D + hidden.size + rows * D) + 128 * 1024
    results = pl.pallas_call(
        functools.partial(kernel, nd, ne, C, S, K),
        out_shape=tuple(pltpu.VMEM(*s) for s in shapes),
        in_specs=[far, far, near, near, far],
        out_specs=(near,) * 4,
        scratch_shapes=[
            vm(hidden.shape, BF16), vm((K, F, vw), BF16), vm((C, N, 2, tok, cw), BF16),
            vm((S, N, 2, tok, cw), BF16),
            vm((N, 2, tall, 128), F32), vm((ne, 8, 128), F32), vm((ne, 8, 128), F32),
            vm((N, 2, tok, F), BF16), vm((N, 2, tok, F), BF16), vm((F, T), BF16), vm((2 * rows, T), BF16),
            vm((T, F), F32),
            vm((summed, 2, rows, cw), BF16), vm((summed, 2, rows, cw), BF16),
            vm((S, rows, cw), BF16), vm((S, rows, cw), BF16),
            vm((summed, rows, cw), BF16), vm((summed, rows, cw), BF16), vm((C, rows, cw), F32),
            vm((summed, rows, cw), F32),
            vm((K, N, tok, vw), BF16), vm((K, N, tok, vw), BF16),
            vm((K, N, tok, vw), BF16), vm((K, N, tok, vw), BF16), vm((K, N, tok, vw), F32),
            sem(1), sem(K), sem(1), sem(K),
            sem(2, N - 1), sem(C, N), sem(1), sem(C),
            sem(2, N - 1), sem(N), sem(1), sem(1), sem(2, N - 1), sem(S, N), sem(1), sem(S),
            sem(1), sem(1), sem(1), sem(1), sem(1), sem(1),
            sem(2), sem(C), sem(1), sem(summed),
            sem(1), sem(K), sem(1), sem(K), sem(3),
        ],
        compiler_params=pltpu.CompilerParams(
            collective_id=0, has_side_effects=True, vmem_limit_bytes=VMEM_BYTES - result_bytes
        ),
    )(hidden, weight_rows, expert_ids.T, gates.T, cotangent)
    mixed, gate_grads, hidden_grads, sums = pl.pallas_call(
        functools.partial(store_kernel, len(shapes)),
        out_shape=tuple(jax.ShapeDtypeStruct(*s) for s in shapes),
        in_specs=[pl.BlockSpec(memory_space=pl.ANY)] * 4,
        out_specs=(far,) * 4,
        scratch_shapes=[sem(len(shapes))],
        compiler_params=pltpu.CompilerParams(vmem_limit_bytes=1024 * 1024),
    )(*results)
    return mixed, gate_grads.T, hidden_grads, sums


def slot_table(expert_ids, experts, capacity):
    flat_ids = expert_ids.reshape(-1)
    choose = (flat_ids[:, None] == jnp.arange(experts, dtype=jnp.int32)[None, :]).astype(jnp.int32)
    earlier = jnp.cumsum(choose, axis=0) - choose
    position = jnp.sum(earlier * choose, axis=1)
    target = flat_ids * capacity + position
    return (target[None, :] == jnp.arange(experts * capacity, dtype=jnp.int32)[:, None]).astype(BF16)


def plain(hidden, weight_rows, expert_ids, gates, cotangent):
    experts = lax.axis_size("expert")
    capacity = hidden.shape[0] // experts
    tok, topk = expert_ids.shape
    width = cotangent.shape[1]
    table = slot_table(expert_ids, experts, capacity)
    weight = lax.all_gather(weight_rows, "dp", axis=0, tiled=True)
    outputs = jnp.dot(hidden, weight, preferred_element_type=F32).astype(BF16)
    back = lax.all_to_all(outputs, "expert", split_axis=0, concat_axis=0, tiled=True)
    picked = lax.dot_general(table, back, (((0,), (0,)), ((), ())), preferred_element_type=F32)
    picked = picked.reshape(tok, topk, width)
    cot32 = cotangent.astype(F32)[:, None, :]
    mixed = jnp.sum(gates[:, :, None] * picked, axis=1).astype(BF16)
    gate_grads = jnp.sum(picked * cot32, axis=2)
    routed = (gates[:, :, None] * cot32).astype(BF16).reshape(-1, width)
    packed = jnp.dot(table, routed, preferred_element_type=F32).astype(BF16)
    grads = lax.all_to_all(packed, "expert", split_axis=0, concat_axis=0, tiled=True)
    hidden_grads = lax.dot_general(
        grads, weight, (((1,), (1,)), ((), ())), preferred_element_type=F32
    ).astype(BF16)
    partial = lax.dot_general(
        hidden, grads, (((0,), (0,)), ((), ())), preferred_element_type=F32
    ).astype(BF16)
    sums = lax.psum_scatter(partial, "dp", scatter_dimension=0, tiled=True)
    return mixed, gate_grads, hidden_grads, sums


def per_device(hidden, w_down, expert_ids, gates, cotangent):
    nd, ne = lax.axis_size("dp"), lax.axis_size("expert")
    rows, width = w_down.shape[1:]
    cap, tok = hidden.shape[0] // ne, expert_ids.shape[0]
    tiled = rows % 16 == 0 and cap % 16 == 0 and tok % 16 == 0 and tok <= 128
    paired = nd == 4 and ne % 2 == 0 and width % 512 == 0
    small = expert_ids.shape[1] <= 8
    body = fused if tiled and paired and small else plain
    mixed, gate_grads, hidden_grads, sums = body(
        hidden, w_down.reshape(rows, width), expert_ids, gates, cotangent
    )
    return mixed, gate_grads, hidden_grads, sums.reshape(1, rows, width)


def solution(mesh):
    split = P(("dp", "expert"), None)
    weights = P("expert", "dp", None)
    return jax.shard_map(
        per_device,
        mesh=mesh,
        in_specs=(split, weights, split, split, split),
        out_specs=(split, split, split, weights),
        check_vma=False,
    )
```

```python
import functools

import jax
import jax.numpy as jnp
from jax import lax
from jax.experimental import pallas as pl
from jax.experimental.pallas import tpu as pltpu
from jax.sharding import PartitionSpec as P

MESH = pl.DeviceIdType.MESH
F32 = jnp.float32
BF16 = jnp.bfloat16


VMEM_BYTES = 67043328


def kernel(
    nd, ne, C, S, K, groups,
    hidden_in, w, ids_in, gates_in, cot,
    mixed, gate_grads, hidden_grads, weight_grads,
    ids, gates, hidden, wfull, cot_all, cot_far, meta, gg_send, gg_recv,
    ht, gh, ght, ght_far, z, wg_send1, wg_recv1, wg_part, wg_recvp, wg_send2, wg_recv2, wg_own, wg_hold,
    mx_send1, mx_recv1, mx_send2, mx_recv2, mx_own,
    wy_r, wf_r, zr, xr, zmr, xmr, cy_r, hy_r, gg_r,
    g1_r, g2_r, m1_r, m2_r, out_w, out_x, out_g, out_t, out_gg, ready,
):
    N = ne // 2
    rows, D = w.shape
    topk, tok = ids.shape
    F = hidden.shape[1]
    cap = hidden.shape[0] // ne
    T, cw, vw = ne * tok, D // C, D // K
    summed = C - S
    a, e = lax.axis_index("dp"), lax.axis_index("expert")
    r, c = a // 2, a % 2
    q, x = e // 2, e % 2

    def to(a2, e2):
        return {"dp": a2, "expert": e2}

    pair_e, pair_c, pair_y = to(a, q * 2 + 1 - x), to(r * 2 + 1 - c, e), to((1 - r) * 2 + c, e)
    ahead, behind = to(a, ((q + 1) % N) * 2 + x), to(a, ((q + N - 1) % N) * 2 + x)
    not_last, not_first = q + 1 < N, q > 0
    onward = ((not_last, ahead), (not_first, behind))

    def copy_of(src, dst, ss, rs, dev):
        return pltpu.make_async_remote_copy(
            src_ref=src, dst_ref=dst, send_sem=ss, recv_sem=rs, device_id=dev, device_id_type=MESH
        )

    def start(src, dst, ss, rs, dev):
        copy_of(src, dst, ss, rs, dev).start()

    def arrived(ref, sem):
        copy_of(ref, ref, sem, sem, pair_e).wait_recv()

    def left(ref, sem):
        copy_of(ref, ref, sem, sem, pair_e).wait_send()

    def w_rows(block):
        return pl.ds(pl.multiple_of(block * rows, rows), rows)

    def cols(j, width=cw):
        return slice(j * width, (j + 1) * width)

    barrier = pltpu.get_barrier_semaphore()
    for dev in (pair_y, pair_c, pair_e):
        pl.semaphore_signal(barrier, inc=1, device_id=dev, device_id_type=MESH)
    for exists, dev in onward:

        @pl.when(exists)
        def _():
            pl.semaphore_signal(barrier, inc=1, device_id=dev, device_id_type=MESH)

    own_ids = pltpu.make_async_copy(ids_in, ids, out_t.at[0])
    own_gates = pltpu.make_async_copy(gates_in, gates, out_g.at[0])
    own_ids.start()
    own_gates.start()
    for j in range(K):
        pltpu.make_async_copy(w.at[:, cols(j, vw)], wfull.at[j, w_rows(a)], out_w.at[0]).start()
    for j in range(C):
        pltpu.make_async_copy(cot.at[:, cols(j)], cot_all.at[j, q, x], out_x.at[0]).start()
    own_h = pltpu.make_async_copy(hidden_in, hidden, out_gg.at[0])
    own_h.start()

    meta[q, x] = jnp.zeros(meta.shape[2:], F32)
    gg_send[...] = jnp.zeros_like(gg_send)
    own_ids.wait()
    own_gates.wait()
    idf = ids[...].astype(F32)
    meta[q, x, 0:topk, 0:tok] = idf
    meta[q, x, topk : 2 * topk, 0:tok] = gates[...]

    mine, theirs = w_rows(a), w_rows((1 - r) * 2 + c)
    pltpu.make_async_copy(wfull.at[:, mine], wfull.at[:, mine], out_w.at[0]).wait()
    own_c = cot_all.at[:, q, x]
    pltpu.make_async_copy(own_c, own_c, out_x.at[0]).wait()
    pl.semaphore_wait(barrier, 3 + not_last.astype(jnp.int32) + not_first.astype(jnp.int32))

    def there(side, d):
        return q + d < N if side else q >= d

    def at(side, d):
        return q + d if side else q - d

    def place(side, d):
        return q + d - 1 if side else d - 1

    def place_next(side, d):
        return q - 1 + d if side else d

    def pass_pair(p, side, d):
        ref = cot_far.at[p, at(side, d)]
        start(ref, ref, out_x.at[0], zr.at[C + p, place_next(side, d)], onward[side][1])

    def pass_cot(i, side, d):
        ref = cot_all.at[i, at(side, d), x]
        start(ref, ref, out_x.at[0], zr.at[i, place_next(side, d)], onward[side][1])

    def across(i, zq):
        ref = cot_all.at[i, zq, x]
        start(ref, ref, out_x.at[0], xr.at[i], pair_e)

    def tell(d):
        for side in range(2):

            @pl.when(there(side, d - 1) & onward[side][0])
            def _():
                pl.semaphore_signal(
                    ready.at[side, d - 2], inc=1, device_id=onward[side][1], device_id_type=MESH
                )

    def hear(d):
        for side in range(2):

            @pl.when(there(side, d))
            def _():
                pl.semaphore_wait(ready.at[side, d - 2], 1)

    def tiles_cross():
        start(meta.at[q, x], meta.at[q, x], out_t.at[0], xmr.at[0], pair_e)

    def tiles_out():
        arrived(meta.at[q, 1 - x], xmr.at[0])
        for d in order:
            start(meta.at[q], meta.at[q], out_t.at[0], zmr.at[0], to(a, ((q + d) % N) * 2 + x))

    def tiles_in():
        arrived(meta.at[0 : N - 1], zmr.at[0])

    def pair_step(p, d):
        if d == 0:
            arrived(cot_far.at[p, q, 1 - x], xr.at[C + p])
        for side in range(2):

            @pl.when(there(side, d) if d else onward[side][0])
            def _():
                if d:
                    arrived(cot_far.at[p, at(side, d)], zr.at[C + p, place(side, d)])
                if 0 < d < N - 1:

                    @pl.when(onward[side][0])
                    def _():
                        pass_pair(p, side, d)

                if d == 0:
                    pass_pair(p, side, d)

    def begin(i):
        for side in range(2):

            @pl.when(onward[side][0])
            def _():
                pass_cot(i, side, 0)

    def step(i, d):
        for side in range(2):

            @pl.when(there(side, d))
            def _():
                arrived(cot_all.at[i, at(side, d), x], zr.at[i, place(side, d)])
                if d < N - 1:

                    @pl.when(onward[side][0])
                    def _():
                        pass_cot(i, side, d)

                across(i, at(side, d))

    def begin_far():
        arrived(cot_far.at[:, q, x], cy_r.at[0])
        for s in range(S):
            ref = cot_far.at[s, q, x]
            start(ref, ref, out_x.at[0], xr.at[C + s], pair_e)

    complete = set()

    def gathered(i):
        if i not in complete:
            complete.add(i)
            arrived(cot_all.at[i, :, 1 - x], xr.at[i])

    order = sorted(range(1, N), key=lambda d: min(d, N - d))

    def send_w(k):
        ref = wfull.at[slice(*groups[k]), mine]
        start(ref, ref, out_w.at[0], wy_r.at[k], pair_y)

    def share_w(k):
        ref = wfull.at[slice(*groups[k]), mine]
        start(ref, ref, out_w.at[0], wf_r.at[k], pair_c)

    def forward_w(k):
        ref = wfull.at[slice(*groups[k]), theirs]
        arrived(ref, wy_r.at[k])
        start(ref, ref, out_w.at[0], wf_r.at[k], pair_c)

    def send_far():
        start(
            cot_all.at[summed:C, q, x], cot_far.at[:, q, x], out_x.at[0], cy_r.at[0], pair_y
        )

    def placer(slot_row):
        return (lax.broadcasted_iota(jnp.int32, (cap, tok), 0).astype(F32) == slot_row).astype(BF16)

    eye = lax.broadcasted_iota(jnp.int32, (tok, tok), 0) == lax.broadcasted_iota(jnp.int32, (tok, tok), 1)

    def to_row(col):
        return jnp.sum(jnp.where(eye, col, 0.0), axis=0, keepdims=True)

    def to_col(row):
        return jnp.sum(jnp.where(eye, row, 0.0), axis=1, keepdims=True)

    def routes():
        upper = (
            lax.broadcasted_iota(jnp.int32, (tok, tok), 0) < lax.broadcasted_iota(jnp.int32, (tok, tok), 1)
        ).astype(BF16)
        chosen, weight = [], []
        for b in range(ne):
            tile = meta[b // 2, b % 2]
            hit = tile[0:topk, 0:tok] == e.astype(F32)
            chosen.append(jnp.sum(jnp.where(hit, 1.0, 0.0), axis=0, keepdims=True))
            weight.append(jnp.sum(jnp.where(hit, tile[topk : 2 * topk, 0:tok], 0.0), axis=0, keepdims=True))
        choose = jnp.concatenate(chosen, axis=0)
        position = jnp.dot(choose.astype(BF16), upper, preferred_element_type=F32)
        slots = jnp.where(choose > 0.0, position, -1.0)
        return [slots[b : b + 1, :] for b in range(ne)], weight

    def pick(slot_rows, gate_rows):
        for b in range(ne):
            rows_b = lax.dot_general(
                placer(slot_rows[b]), hidden[b * cap : (b + 1) * cap, :], (((0,), (0,)), ((), ())),
                preferred_element_type=F32,
            )
            ht[b // 2, b % 2] = rows_b.astype(BF16)
            gh[b // 2, b % 2] = (to_col(gate_rows[b]) * rows_b).astype(BF16)
        ght[...] = gh[...].reshape(T, F).astype(F32).T.astype(BF16)

    def send_rows():
        there_rows = pl.ds(pl.multiple_of((1 - r) * 2 * rows, 2 * rows), 2 * rows)
        start(ght.at[there_rows], ght_far, out_g.at[0], hy_r.at[0], pair_y)

    def block_of(j, b):
        return jnp.dot(ght[w_rows(b), :], cot_all[j].reshape(T, cw), preferred_element_type=F32)

    def begin_grads(j):
        gathered(j)
        for k in range(2):
            wg_send1[j, k] = block_of(j, ((r + k) % 2) * 2 + 1 - c).astype(BF16)
        start(wg_send1.at[j], wg_recv1.at[j], out_g.at[0], g1_r.at[j], pair_c)
        wg_hold[j] = block_of(j, (1 - r) * 2 + c)
        wg_own[j] = block_of(j, r * 2 + c)

    def pass_grads(j):
        arrived(wg_recv1.at[j], g1_r.at[j])
        wg_send2[j] = (wg_hold[j] + wg_recv1[j, 1].astype(F32)).astype(BF16)
        start(wg_send2.at[j], wg_recv2.at[j], out_g.at[0], g2_r.at[j], pair_y)

    def full_grads(j):
        s = j - summed
        gathered(j)
        if s == 0:
            arrived(ght_far, hy_r.at[0])

        def both(core):
            other = jnp.dot(
                ght_far[w_rows(core), :], cot_far[s].reshape(T, cw), preferred_element_type=F32
            )
            return block_of(j, r * 2 + core) + other

        wg_part[s] = both(1 - c).astype(BF16)
        start(wg_part.at[s], wg_recvp.at[s], out_g.at[0], g1_r.at[j], pair_c)
        wg_own[j] = both(c)

    def out_part(k):
        piece = slice(*groups[k])
        arrived(wfull.at[piece, 0 : 2 * rows], wf_r.at[k])
        lhs = gh[:, pl.ds(1 - x, 1)].reshape(N * tok, F)
        for j in range(*groups[k]):
            val = jnp.dot(lhs, wfull[j], preferred_element_type=F32)
            mx_send1[j] = val.astype(BF16).reshape(N, tok, vw)
        start(mx_send1.at[piece], mx_recv1.at[piece], out_x.at[0], m1_r.at[k], pair_e)
        lhs = gh[:, pl.ds(x, 1)].reshape(N * tok, F)
        for j in range(*groups[k]):
            val = jnp.dot(lhs, wfull[j], preferred_element_type=F32)
            mx_own[j] = val.reshape(N, tok, vw)

    def z_part(k):
        for j in range(*groups[k]):
            i = j * vw // cw
            gathered(i)
            part = cot_all[i, :, :, :, cols(j % (cw // vw), vw)].reshape(T, vw)
            val = lax.dot_general(part, wfull[j], (((1,), (1,)), ((), ())), preferred_element_type=F32)
            z[...] = val if j == 0 else z[...] + val

    early = groups[-2][0]

    def mix_part(k):
        piece = slice(*groups[k])
        arrived(mx_recv1.at[piece], m1_r.at[k])
        sem = m2_r.at[max(0, k - len(groups) + 3)]
        for d in order:
            o = (q + d) % N
            for j in range(*groups[k]):
                mx_send2[j, o] = (mx_own[j, o] + mx_recv1[j, o].astype(F32)).astype(BF16)
            start(mx_send2.at[piece, o], mx_recv2.at[piece, q], out_x.at[0], sem, to(a, o * 2 + x))

    def hidden_part(slot_rows, gate_rows):
        for b in range(ne):
            zb = z[b * tok : (b + 1) * tok, :]
            gg_col = jnp.sum(ht[b // 2, b % 2].astype(F32) * zb, axis=1, keepdims=True)
            gg_send[b, 0:1, 0:tok] = to_row(gg_col)
            scaled = (to_col(gate_rows[b]) * zb).astype(BF16)
            hidden_grads[b * cap : (b + 1) * cap, :] = jnp.dot(
                placer(slot_rows[b]), scaled, preferred_element_type=F32
            ).astype(BF16)
        for d in range(1, ne):
            o = (e + d) % ne
            start(gg_send.at[o], gg_recv.at[e], out_gg.at[0], gg_r.at[0], to(a, o))
        gg_recv[e] = gg_send[e]

    def finish_mixed(k):
        first, last = (0, early) if k == 0 else groups[k - 3]
        arrived(mx_recv2.at[first:last, 0 : N - 1], m2_r.at[k])
        for j in range(first, last):
            total = mx_own[j, q] + mx_recv1[j, q].astype(F32)
            for d in order:
                total = total + mx_recv2[j, (q - d + N) % N].astype(F32)
            mixed[:, cols(j, vw)] = total.astype(BF16)

    def finish_gates():
        arrived(gg_recv.at[0 : ne - 1], gg_r.at[0])
        for k in range(topk):
            row = jnp.zeros((1, tok), F32)
            for b in range(ne):
                row = row + jnp.where(idf[k : k + 1, :] == float(b), gg_recv[b, 0:1, 0:tok], 0.0)
            gate_grads[k : k + 1, :] = row

    def finish_grads(j):
        if j >= summed:
            arrived(wg_recvp.at[j - summed], g1_r.at[j])
            weight_grads[:, cols(j)] = (wg_own[j] + wg_recvp[j - summed].astype(F32)).astype(BF16)
            return
        val = wg_own[j] + wg_recv1[j, 0].astype(F32)
        arrived(wg_recv2.at[j], g2_r.at[j])
        weight_grads[:, cols(j)] = (val + wg_recv2[j].astype(F32)).astype(BF16)

    tiles_cross()
    send_far()
    for k in range(len(groups)):
        send_w(k)
    for j in range(C):
        across(j, q)
    begin(0)
    begin(1)
    for d in range(2, N):
        tell(d)
        if d == 2:
            for k in range(len(groups)):
                share_w(k)
        hear(d)
    tiles_out()
    begin(2)
    begin(3)
    begin_far()
    step(0, 1)
    step(1, 1)
    step(2, 1)
    step(3, 1)
    pair_step(0, 0)
    forward_w(0)
    step(0, 2)
    step(1, 2)
    own_h.wait()
    tiles_in()
    slot_rows, gate_rows = routes()
    pick(slot_rows, gate_rows)
    send_rows()
    out_part(0)
    step(2, 2)
    step(3, 2)
    pair_step(1, 0)
    step(0, 3)
    forward_w(1)
    step(1, 3)
    out_part(1)
    step(2, 3)
    step(3, 3)
    pair_step(0, 1)
    forward_w(2)
    mix_part(0)
    pair_step(1, 1)
    forward_w(3)
    out_part(2)
    begin_grads(0)
    forward_w(4)
    out_part(3)
    mix_part(1)
    forward_w(5)
    begin_grads(1)
    pass_grads(0)
    out_part(4)
    pair_step(0, 2)
    mix_part(2)
    out_part(5)
    pair_step(1, 2)
    mix_part(3)
    z_part(0)
    z_part(1)
    z_part(2)
    z_part(3)
    z_part(4)
    z_part(5)
    hidden_part(slot_rows, gate_rows)
    mix_part(4)
    pass_grads(1)
    pair_step(0, 3)
    mix_part(5)
    full_grads(2)
    pair_step(1, 3)
    full_grads(3)
    finish_mixed(0)
    finish_gates()
    finish_grads(2)
    finish_grads(0)
    finish_mixed(1)
    finish_grads(1)
    finish_grads(3)
    finish_mixed(2)

    left(wfull.at[:, 0 : 3 * rows], out_w.at[0])
    left(wfull.at[:, 0 : 2 * rows + 2 * rows * T // D], out_g.at[0])
    for inner in range(2):

        @pl.when((not_first & not_last) if inner else ~(not_first & not_last))
        def _():
            left(wfull.at[:, 0 : 3 * N * tok + 2 * tok * (N + 1 if inner else 1)], out_x.at[0])

    left(gg_recv.at[0 : 2 * N - 1], out_t.at[0])
    left(gg_send.at[0 : ne - 1], out_gg.at[0])


def store_kernel(count, *refs):
    sems = refs[-1]
    copies = [pltpu.make_async_copy(refs[i], refs[count + i], sems.at[i]) for i in range(count)]
    for copy in copies:
        copy.start()
    for copy in copies:
        copy.wait()


def fused(hidden, weight_rows, expert_ids, gates, cotangent):
    nd, ne = lax.axis_size("dp"), lax.axis_size("expert")
    rows, D = weight_rows.shape
    tok, topk = expert_ids.shape
    F = hidden.shape[1]
    T, N = ne * tok, ne // 2
    C, S, K = 4, 2, 8
    groups = ((0, 2), (2, 4), (4, 5), (5, 6), (6, 7), (7, 8))
    G = len(groups)
    cw, vw, summed = D // C, D // K, C - S
    vm = pltpu.VMEM
    sem = lambda *n: pltpu.SemaphoreType.DMA(tuple(max(i, 1) for i in n))
    near, far = pl.BlockSpec(memory_space=pltpu.VMEM), pl.BlockSpec(memory_space=pltpu.HBM)
    shapes = [((tok, D), BF16), ((topk, tok), F32), (hidden.shape, BF16), ((rows, D), BF16)]
    tall = -(-2 * topk // 8) * 8
    result_bytes = 2 * (tok * D + hidden.size + rows * D) + 128 * 1024
    results = pl.pallas_call(
        functools.partial(kernel, nd, ne, C, S, K, groups),
        out_shape=tuple(pltpu.VMEM(*s) for s in shapes),
        in_specs=[far] * 5,
        out_specs=(near,) * 4,
        scratch_shapes=[
            vm((topk, tok), jnp.int32), vm((topk, tok), F32), vm(hidden.shape, BF16), vm((K, F, vw), BF16), vm((C, N, 2, tok, cw), BF16),
            vm((S, N, 2, tok, cw), BF16),
            vm((N, 2, tall, 128), F32), vm((ne, 8, 128), F32), vm((ne, 8, 128), F32),
            vm((N, 2, tok, F), BF16), vm((N, 2, tok, F), BF16), vm((F, T), BF16), vm((2 * rows, T), BF16),
            vm((T, F), F32),
            vm((summed, 2, rows, cw), BF16), vm((summed, 2, rows, cw), BF16),
            vm((S, rows, cw), BF16), vm((S, rows, cw), BF16),
            vm((summed, rows, cw), BF16), vm((summed, rows, cw), BF16), vm((C, rows, cw), F32),
            vm((summed, rows, cw), F32),
            vm((K, N, tok, vw), BF16), vm((K, N, tok, vw), BF16),
            vm((K, N, tok, vw), BF16), vm((K, N, tok, vw), BF16), vm((K, N, tok, vw), F32),
            sem(G), sem(G), sem(C + S, N - 1), sem(C + S), sem(1), sem(1), sem(1), sem(1), sem(1),
            sem(C), sem(summed), sem(G), sem(3), sem(1), sem(1), sem(1), sem(1), sem(1),
            pltpu.SemaphoreType.REGULAR((2, max(N - 2, 1))),
        ],
        compiler_params=pltpu.CompilerParams(
            collective_id=0, has_side_effects=True, vmem_limit_bytes=VMEM_BYTES - result_bytes
        ),
    )(hidden, weight_rows, expert_ids.T, gates.T, cotangent)
    mixed, gate_grads, hidden_grads, sums = pl.pallas_call(
        functools.partial(store_kernel, len(shapes)),
        out_shape=tuple(jax.ShapeDtypeStruct(*s) for s in shapes),
        in_specs=[pl.BlockSpec(memory_space=pl.ANY)] * 4,
        out_specs=(far,) * 4,
        scratch_shapes=[sem(len(shapes))],
        compiler_params=pltpu.CompilerParams(vmem_limit_bytes=1024 * 1024),
    )(*results)
    return mixed, gate_grads.T, hidden_grads, sums


def slot_table(expert_ids, experts, capacity):
    flat_ids = expert_ids.reshape(-1)
    choose = (flat_ids[:, None] == jnp.arange(experts, dtype=jnp.int32)[None, :]).astype(jnp.int32)
    earlier = jnp.cumsum(choose, axis=0) - choose
    position = jnp.sum(earlier * choose, axis=1)
    target = flat_ids * capacity + position
    return (target[None, :] == jnp.arange(experts * capacity, dtype=jnp.int32)[:, None]).astype(BF16)


def plain(hidden, weight_rows, expert_ids, gates, cotangent):
    experts = lax.axis_size("expert")
    capacity = hidden.shape[0] // experts
    tok, topk = expert_ids.shape
    width = cotangent.shape[1]
    table = slot_table(expert_ids, experts, capacity)
    weight = lax.all_gather(weight_rows, "dp", axis=0, tiled=True)
    outputs = jnp.dot(hidden, weight, preferred_element_type=F32).astype(BF16)
    back = lax.all_to_all(outputs, "expert", split_axis=0, concat_axis=0, tiled=True)
    picked = lax.dot_general(table, back, (((0,), (0,)), ((), ())), preferred_element_type=F32)
    picked = picked.reshape(tok, topk, width)
    cot32 = cotangent.astype(F32)[:, None, :]
    mixed = jnp.sum(gates[:, :, None] * picked, axis=1).astype(BF16)
    gate_grads = jnp.sum(picked * cot32, axis=2)
    routed = (gates[:, :, None] * cot32).astype(BF16).reshape(-1, width)
    packed = jnp.dot(table, routed, preferred_element_type=F32).astype(BF16)
    grads = lax.all_to_all(packed, "expert", split_axis=0, concat_axis=0, tiled=True)
    hidden_grads = lax.dot_general(
        grads, weight, (((1,), (1,)), ((), ())), preferred_element_type=F32
    ).astype(BF16)
    partial = lax.dot_general(
        hidden, grads, (((0,), (0,)), ((), ())), preferred_element_type=F32
    ).astype(BF16)
    sums = lax.psum_scatter(partial, "dp", scatter_dimension=0, tiled=True)
    return mixed, gate_grads, hidden_grads, sums


def per_device(hidden, w_down, expert_ids, gates, cotangent):
    nd, ne = lax.axis_size("dp"), lax.axis_size("expert")
    rows, width = w_down.shape[1:]
    cap, tok = hidden.shape[0] // ne, expert_ids.shape[0]
    tiled = rows % 16 == 0 and cap % 16 == 0 and tok % 16 == 0 and tok <= 128
    paired = nd == 4 and ne % 2 == 0 and width % 512 == 0
    small = expert_ids.shape[1] <= 8
    body = fused if tiled and paired and small else plain
    mixed, gate_grads, hidden_grads, sums = body(
        hidden, w_down.reshape(rows, width), expert_ids, gates, cotangent
    )
    return mixed, gate_grads, hidden_grads, sums.reshape(1, rows, width)


def solution(mesh):
    split = P(("dp", "expert"), None)
    weights = P("expert", "dp", None)
    return jax.shard_map(
        per_device,
        mesh=mesh,
        in_specs=(split, weights, split, split, split),
        out_specs=(split, split, split, weights),
        check_vma=False,
    )
```

```python
import functools

import jax
import jax.numpy as jnp
from jax import lax
from jax.experimental import pallas as pl
from jax.experimental.pallas import tpu as pltpu
from jax.sharding import PartitionSpec as P

MESH = pl.DeviceIdType.MESH
F32 = jnp.float32
BF16 = jnp.bfloat16


VMEM_BYTES = 67043328


def kernel(
    nd, ne, C, S, K, groups,
    hidden_in, w, ids_in, gates_in, cot,
    mixed, gate_grads, hidden_grads, weight_grads,
    ids, gates, hidden, wfull, cot_all, cot_far, meta, gg_send, gg_recv,
    ht, gh, ght, ght_far, z, wg_send1, wg_recv1, wg_part, wg_recvp, wg_send2, wg_recv2, wg_own, wg_hold,
    mx_send1, mx_recv1, mx_send2, mx_recv2, mx_own,
    wy_r, wf_r, zr, xr, zmr, xmr, cy_r, hy_r, gg_r,
    g1_r, g2_r, m1_r, m2_r, out_w, out_x, out_g, out_t, out_gg, ready,
):
    N = ne // 2
    rows, D = w.shape
    topk, tok = ids.shape
    F = hidden.shape[1]
    cap = hidden.shape[0] // ne
    T, cw, vw = ne * tok, D // C, D // K
    summed = C - S
    a, e = lax.axis_index("dp"), lax.axis_index("expert")
    r, c = a // 2, a % 2
    q, x = e // 2, e % 2

    def to(a2, e2):
        return {"dp": a2, "expert": e2}

    pair_e, pair_c, pair_y = to(a, q * 2 + 1 - x), to(r * 2 + 1 - c, e), to((1 - r) * 2 + c, e)
    ahead, behind = to(a, ((q + 1) % N) * 2 + x), to(a, ((q + N - 1) % N) * 2 + x)
    not_last, not_first = q + 1 < N, q > 0
    onward = ((not_last, ahead), (not_first, behind))

    def copy_of(src, dst, ss, rs, dev):
        return pltpu.make_async_remote_copy(
            src_ref=src, dst_ref=dst, send_sem=ss, recv_sem=rs, device_id=dev, device_id_type=MESH
        )

    def start(src, dst, ss, rs, dev):
        copy_of(src, dst, ss, rs, dev).start()

    def arrived(ref, sem):
        copy_of(ref, ref, sem, sem, pair_e).wait_recv()

    def left(ref, sem):
        copy_of(ref, ref, sem, sem, pair_e).wait_send()

    def w_rows(block):
        return pl.ds(pl.multiple_of(block * rows, rows), rows)

    def cols(j, width=cw):
        return slice(j * width, (j + 1) * width)

    barrier = pltpu.get_barrier_semaphore()
    for dev in (pair_y, pair_c, pair_e):
        pl.semaphore_signal(barrier, inc=1, device_id=dev, device_id_type=MESH)
    for exists, dev in onward:

        @pl.when(exists)
        def _():
            pl.semaphore_signal(barrier, inc=1, device_id=dev, device_id_type=MESH)

    own_ids = pltpu.make_async_copy(ids_in, ids, out_t.at[0])
    own_gates = pltpu.make_async_copy(gates_in, gates, out_g.at[0])
    own_ids.start()
    own_gates.start()
    for j in range(K):
        pltpu.make_async_copy(w.at[:, cols(j, vw)], wfull.at[j, w_rows(a)], out_w.at[0]).start()
    for j in range(C):
        pltpu.make_async_copy(cot.at[:, cols(j)], cot_all.at[j, q, x], out_x.at[0]).start()
    own_h = pltpu.make_async_copy(hidden_in, hidden, out_gg.at[0])
    own_h.start()

    meta[q, x] = jnp.zeros(meta.shape[2:], F32)
    gg_send[...] = jnp.zeros_like(gg_send)
    own_ids.wait()
    own_gates.wait()
    idf = ids[...].astype(F32)
    meta[q, x, 0:topk, 0:tok] = idf
    meta[q, x, topk : 2 * topk, 0:tok] = gates[...]

    mine, theirs = w_rows(a), w_rows((1 - r) * 2 + c)
    pltpu.make_async_copy(wfull.at[:, mine], wfull.at[:, mine], out_w.at[0]).wait()
    own_c = cot_all.at[:, q, x]
    pltpu.make_async_copy(own_c, own_c, out_x.at[0]).wait()
    pl.semaphore_wait(barrier, 3 + not_last.astype(jnp.int32) + not_first.astype(jnp.int32))

    def there(side, d):
        return q + d < N if side else q >= d

    def at(side, d):
        return q + d if side else q - d

    def place(side, d):
        return q + d - 1 if side else d - 1

    def place_next(side, d):
        return q - 1 + d if side else d

    def pass_pair(p, side, d):
        ref = cot_far.at[p, at(side, d)]
        start(ref, ref, out_x.at[0], zr.at[C + p, place_next(side, d)], onward[side][1])

    def pass_cot(i, side, d):
        ref = cot_all.at[i, at(side, d), x]
        start(ref, ref, out_x.at[0], zr.at[i, place_next(side, d)], onward[side][1])

    def across(i, zq):
        ref = cot_all.at[i, zq, x]
        start(ref, ref, out_x.at[0], xr.at[i], pair_e)

    def tell(d):
        for side in range(2):

            @pl.when(there(side, d - 1) & onward[side][0])
            def _():
                pl.semaphore_signal(
                    ready.at[side, d - 2], inc=1, device_id=onward[side][1], device_id_type=MESH
                )

    def hear(d):
        for side in range(2):

            @pl.when(there(side, d))
            def _():
                pl.semaphore_wait(ready.at[side, d - 2], 1)

    def tiles_cross():
        start(meta.at[q, x], meta.at[q, x], out_t.at[0], xmr.at[0], pair_e)

    def tiles_out():
        arrived(meta.at[q, 1 - x], xmr.at[0])
        for d in order:
            start(meta.at[q], meta.at[q], out_t.at[0], zmr.at[0], to(a, ((q + d) % N) * 2 + x))

    def tiles_in():
        arrived(meta.at[0 : N - 1], zmr.at[0])

    def pair_step(p, d):
        if d == 0:
            arrived(cot_far.at[p, q, 1 - x], xr.at[C + p])
        for side in range(2):

            @pl.when(there(side, d) if d else onward[side][0])
            def _():
                if d:
                    arrived(cot_far.at[p, at(side, d)], zr.at[C + p, place(side, d)])
                if 0 < d < N - 1:

                    @pl.when(onward[side][0])
                    def _():
                        pass_pair(p, side, d)

                if d == 0:
                    pass_pair(p, side, d)

    def begin(i):
        for side in range(2):

            @pl.when(onward[side][0])
            def _():
                pass_cot(i, side, 0)

    def step(i, d):
        for side in range(2):

            @pl.when(there(side, d))
            def _():
                arrived(cot_all.at[i, at(side, d), x], zr.at[i, place(side, d)])
                if d < N - 1:

                    @pl.when(onward[side][0])
                    def _():
                        pass_cot(i, side, d)

                across(i, at(side, d))

    def begin_far():
        arrived(cot_far.at[:, q, x], cy_r.at[0])
        for s in range(S):
            ref = cot_far.at[s, q, x]
            start(ref, ref, out_x.at[0], xr.at[C + s], pair_e)

    complete = set()

    def gathered(i):
        if i not in complete:
            complete.add(i)
            arrived(cot_all.at[i, :, 1 - x], xr.at[i])

    order = sorted(range(1, N), key=lambda d: min(d, N - d))

    def send_w(k):
        ref = wfull.at[slice(*groups[k]), mine]
        start(ref, ref, out_w.at[0], wy_r.at[k], pair_y)

    def share_w(k):
        ref = wfull.at[slice(*groups[k]), mine]
        start(ref, ref, out_w.at[0], wf_r.at[k], pair_c)

    def forward_w(k):
        ref = wfull.at[slice(*groups[k]), theirs]
        arrived(ref, wy_r.at[k])
        start(ref, ref, out_w.at[0], wf_r.at[k], pair_c)

    def send_far():
        start(
            cot_all.at[summed:C, q, x], cot_far.at[:, q, x], out_x.at[0], cy_r.at[0], pair_y
        )

    def placer(slot_row):
        return (lax.broadcasted_iota(jnp.int32, (cap, tok), 0).astype(F32) == slot_row).astype(BF16)

    eye = lax.broadcasted_iota(jnp.int32, (tok, tok), 0) == lax.broadcasted_iota(jnp.int32, (tok, tok), 1)

    def to_row(col):
        return jnp.sum(jnp.where(eye, col, 0.0), axis=0, keepdims=True)

    def to_col(row):
        return jnp.sum(jnp.where(eye, row, 0.0), axis=1, keepdims=True)

    def routes():
        upper = (
            lax.broadcasted_iota(jnp.int32, (tok, tok), 0) < lax.broadcasted_iota(jnp.int32, (tok, tok), 1)
        ).astype(BF16)
        chosen, weight = [], []
        for b in range(ne):
            tile = meta[b // 2, b % 2]
            hit = tile[0:topk, 0:tok] == e.astype(F32)
            chosen.append(jnp.sum(jnp.where(hit, 1.0, 0.0), axis=0, keepdims=True))
            weight.append(jnp.sum(jnp.where(hit, tile[topk : 2 * topk, 0:tok], 0.0), axis=0, keepdims=True))
        choose = jnp.concatenate(chosen, axis=0)
        position = jnp.dot(choose.astype(BF16), upper, preferred_element_type=F32)
        slots = jnp.where(choose > 0.0, position, -1.0)
        return [slots[b : b + 1, :] for b in range(ne)], weight

    def pick(slot_rows, gate_rows):
        for b in range(ne):
            rows_b = lax.dot_general(
                placer(slot_rows[b]), hidden[b * cap : (b + 1) * cap, :], (((0,), (0,)), ((), ())),
                preferred_element_type=F32,
            )
            ht[b // 2, b % 2] = rows_b.astype(BF16)
            gh[b // 2, b % 2] = (to_col(gate_rows[b]) * rows_b).astype(BF16)
        ght[...] = gh[...].reshape(T, F).astype(F32).T.astype(BF16)

    def send_rows():
        there_rows = pl.ds(pl.multiple_of((1 - r) * 2 * rows, 2 * rows), 2 * rows)
        start(ght.at[there_rows], ght_far, out_g.at[0], hy_r.at[0], pair_y)

    def block_of(j, b):
        return jnp.dot(ght[w_rows(b), :], cot_all[j].reshape(T, cw), preferred_element_type=F32)

    def begin_grads(j):
        gathered(j)
        for k in range(2):
            wg_send1[j, k] = block_of(j, ((r + k) % 2) * 2 + 1 - c).astype(BF16)
        start(wg_send1.at[j], wg_recv1.at[j], out_g.at[0], g1_r.at[j], pair_c)
        wg_hold[j] = block_of(j, (1 - r) * 2 + c)
        wg_own[j] = block_of(j, r * 2 + c)

    def pass_grads(j):
        arrived(wg_recv1.at[j], g1_r.at[j])
        wg_send2[j] = (wg_hold[j] + wg_recv1[j, 1].astype(F32)).astype(BF16)
        start(wg_send2.at[j], wg_recv2.at[j], out_g.at[0], g2_r.at[j], pair_y)

    def full_grads(j):
        s = j - summed
        gathered(j)
        if s == 0:
            arrived(ght_far, hy_r.at[0])

        def both(core):
            other = jnp.dot(
                ght_far[w_rows(core), :], cot_far[s].reshape(T, cw), preferred_element_type=F32
            )
            return block_of(j, r * 2 + core) + other

        wg_part[s] = both(1 - c).astype(BF16)
        start(wg_part.at[s], wg_recvp.at[s], out_g.at[0], g1_r.at[j], pair_c)
        wg_own[j] = both(c)

    def out_part(k):
        piece = slice(*groups[k])
        arrived(wfull.at[piece, 0 : 2 * rows], wf_r.at[k])
        lhs = gh[:, pl.ds(1 - x, 1)].reshape(N * tok, F)
        for j in range(*groups[k]):
            val = jnp.dot(lhs, wfull[j], preferred_element_type=F32)
            mx_send1[j] = val.astype(BF16).reshape(N, tok, vw)
        start(mx_send1.at[piece], mx_recv1.at[piece], out_x.at[0], m1_r.at[k], pair_e)
        lhs = gh[:, pl.ds(x, 1)].reshape(N * tok, F)
        for j in range(*groups[k]):
            val = jnp.dot(lhs, wfull[j], preferred_element_type=F32)
            mx_own[j] = val.reshape(N, tok, vw)

    def z_part(k):
        for j in range(*groups[k]):
            i = j * vw // cw
            gathered(i)
            part = cot_all[i, :, :, :, cols(j % (cw // vw), vw)].reshape(T, vw)
            val = lax.dot_general(part, wfull[j], (((1,), (1,)), ((), ())), preferred_element_type=F32)
            z[...] = val if j == 0 else z[...] + val

    early = groups[-2][0]

    def mix_part(k):
        piece = slice(*groups[k])
        arrived(mx_recv1.at[piece], m1_r.at[k])
        sem = m2_r.at[max(0, k - len(groups) + 3)]
        for d in order:
            o = (q + d) % N
            for j in range(*groups[k]):
                mx_send2[j, o] = (mx_own[j, o] + mx_recv1[j, o].astype(F32)).astype(BF16)
            start(mx_send2.at[piece, o], mx_recv2.at[piece, q], out_x.at[0], sem, to(a, o * 2 + x))

    def hidden_part(slot_rows, gate_rows):
        for b in range(ne):
            zb = z[b * tok : (b + 1) * tok, :]
            gg_col = jnp.sum(ht[b // 2, b % 2].astype(F32) * zb, axis=1, keepdims=True)
            gg_send[b, 0:1, 0:tok] = to_row(gg_col)
            scaled = (to_col(gate_rows[b]) * zb).astype(BF16)
            hidden_grads[b * cap : (b + 1) * cap, :] = jnp.dot(
                placer(slot_rows[b]), scaled, preferred_element_type=F32
            ).astype(BF16)
        for d in range(1, ne):
            o = (e + d) % ne
            start(gg_send.at[o], gg_recv.at[e], out_gg.at[0], gg_r.at[0], to(a, o))
        gg_recv[e] = gg_send[e]

    def finish_mixed(k):
        first, last = (0, early) if k == 0 else groups[k - 3]
        arrived(mx_recv2.at[first:last, 0 : N - 1], m2_r.at[k])
        for j in range(first, last):
            total = mx_own[j, q] + mx_recv1[j, q].astype(F32)
            for d in order:
                total = total + mx_recv2[j, (q - d + N) % N].astype(F32)
            mixed[:, cols(j, vw)] = total.astype(BF16)

    def finish_gates():
        arrived(gg_recv.at[0 : ne - 1], gg_r.at[0])
        for k in range(topk):
            row = jnp.zeros((1, tok), F32)
            for b in range(ne):
                row = row + jnp.where(idf[k : k + 1, :] == float(b), gg_recv[b, 0:1, 0:tok], 0.0)
            gate_grads[k : k + 1, :] = row

    def finish_grads(j):
        if j >= summed:
            arrived(wg_recvp.at[j - summed], g1_r.at[j])
            weight_grads[:, cols(j)] = (wg_own[j] + wg_recvp[j - summed].astype(F32)).astype(BF16)
            return
        val = wg_own[j] + wg_recv1[j, 0].astype(F32)
        arrived(wg_recv2.at[j], g2_r.at[j])
        weight_grads[:, cols(j)] = (val + wg_recv2[j].astype(F32)).astype(BF16)

    tiles_cross()
    send_far()
    for k in range(len(groups)):
        send_w(k)
    for j in range(C):
        across(j, q)
    begin(0)
    begin(1)
    begin(2)
    for d in range(2, N):
        tell(d)
        if d == 2:
            for k in range(len(groups)):
                share_w(k)
        hear(d)
    tiles_out()
    begin(3)
    step(0, 1)
    step(1, 1)
    begin_far()
    step(2, 1)
    step(3, 1)
    step(0, 2)
    forward_w(0)
    step(1, 2)
    pair_step(0, 0)
    own_h.wait()
    tiles_in()
    slot_rows, gate_rows = routes()
    pick(slot_rows, gate_rows)
    send_rows()
    out_part(0)
    step(2, 2)
    step(3, 2)
    step(0, 3)
    forward_w(1)
    pair_step(1, 0)
    step(1, 3)
    out_part(1)
    step(2, 3)
    step(3, 3)
    pair_step(0, 1)
    forward_w(2)
    mix_part(0)
    pair_step(1, 1)
    forward_w(3)
    out_part(2)
    begin_grads(0)
    forward_w(4)
    out_part(3)
    mix_part(1)
    forward_w(5)
    out_part(4)
    pair_step(0, 2)
    begin_grads(1)
    pass_grads(0)
    mix_part(2)
    out_part(5)
    pair_step(1, 2)
    mix_part(3)
    pass_grads(1)
    z_part(0)
    z_part(1)
    z_part(2)
    mix_part(4)
    z_part(3)
    z_part(4)
    z_part(5)
    hidden_part(slot_rows, gate_rows)
    mix_part(5)
    pair_step(0, 3)
    full_grads(2)
    pair_step(1, 3)
    full_grads(3)
    finish_mixed(0)
    finish_gates()
    finish_grads(2)
    finish_grads(0)
    finish_mixed(1)
    finish_grads(1)
    finish_grads(3)
    finish_mixed(2)

    left(wfull.at[:, 0 : 3 * rows], out_w.at[0])
    left(wfull.at[:, 0 : 2 * rows + 2 * rows * T // D], out_g.at[0])
    for inner in range(2):

        @pl.when((not_first & not_last) if inner else ~(not_first & not_last))
        def _():
            left(wfull.at[:, 0 : 3 * N * tok + 2 * tok * (N + 1 if inner else 1)], out_x.at[0])

    left(gg_recv.at[0 : 2 * N - 1], out_t.at[0])
    left(gg_send.at[0 : ne - 1], out_gg.at[0])


def store_kernel(count, *refs):
    sems = refs[-1]
    copies = [pltpu.make_async_copy(refs[i], refs[count + i], sems.at[i]) for i in range(count)]
    for copy in copies:
        copy.start()
    for copy in copies:
        copy.wait()


def fused(hidden, weight_rows, expert_ids, gates, cotangent):
    nd, ne = lax.axis_size("dp"), lax.axis_size("expert")
    rows, D = weight_rows.shape
    tok, topk = expert_ids.shape
    F = hidden.shape[1]
    T, N = ne * tok, ne // 2
    C, S, K = 4, 2, 8
    groups = ((0, 2), (2, 4), (4, 5), (5, 6), (6, 7), (7, 8))
    G = len(groups)
    cw, vw, summed = D // C, D // K, C - S
    vm = pltpu.VMEM
    sem = lambda *n: pltpu.SemaphoreType.DMA(tuple(max(i, 1) for i in n))
    near, far = pl.BlockSpec(memory_space=pltpu.VMEM), pl.BlockSpec(memory_space=pltpu.HBM)
    shapes = [((tok, D), BF16), ((topk, tok), F32), (hidden.shape, BF16), ((rows, D), BF16)]
    tall = -(-2 * topk // 8) * 8
    result_bytes = 2 * (tok * D + hidden.size + rows * D) + 128 * 1024
    results = pl.pallas_call(
        functools.partial(kernel, nd, ne, C, S, K, groups),
        out_shape=tuple(pltpu.VMEM(*s) for s in shapes),
        in_specs=[far] * 5,
        out_specs=(near,) * 4,
        scratch_shapes=[
            vm((topk, tok), jnp.int32), vm((topk, tok), F32), vm(hidden.shape, BF16), vm((K, F, vw), BF16), vm((C, N, 2, tok, cw), BF16),
            vm((S, N, 2, tok, cw), BF16),
            vm((N, 2, tall, 128), F32), vm((ne, 8, 128), F32), vm((ne, 8, 128), F32),
            vm((N, 2, tok, F), BF16), vm((N, 2, tok, F), BF16), vm((F, T), BF16), vm((2 * rows, T), BF16),
            vm((T, F), F32),
            vm((summed, 2, rows, cw), BF16), vm((summed, 2, rows, cw), BF16),
            vm((S, rows, cw), BF16), vm((S, rows, cw), BF16),
            vm((summed, rows, cw), BF16), vm((summed, rows, cw), BF16), vm((C, rows, cw), F32),
            vm((summed, rows, cw), F32),
            vm((K, N, tok, vw), BF16), vm((K, N, tok, vw), BF16),
            vm((K, N, tok, vw), BF16), vm((K, N, tok, vw), BF16), vm((K, N, tok, vw), F32),
            sem(G), sem(G), sem(C + S, N - 1), sem(C + S), sem(1), sem(1), sem(1), sem(1), sem(1),
            sem(C), sem(summed), sem(G), sem(3), sem(1), sem(1), sem(1), sem(1), sem(1),
            pltpu.SemaphoreType.REGULAR((2, max(N - 2, 1))),
        ],
        compiler_params=pltpu.CompilerParams(
            collective_id=0, has_side_effects=True, vmem_limit_bytes=VMEM_BYTES - result_bytes
        ),
    )(hidden, weight_rows, expert_ids.T, gates.T, cotangent)
    mixed, gate_grads, hidden_grads, sums = pl.pallas_call(
        functools.partial(store_kernel, len(shapes)),
        out_shape=tuple(jax.ShapeDtypeStruct(*s) for s in shapes),
        in_specs=[pl.BlockSpec(memory_space=pl.ANY)] * 4,
        out_specs=(far,) * 4,
        scratch_shapes=[sem(len(shapes))],
        compiler_params=pltpu.CompilerParams(vmem_limit_bytes=1024 * 1024),
    )(*results)
    return mixed, gate_grads.T, hidden_grads, sums


def slot_table(expert_ids, experts, capacity):
    flat_ids = expert_ids.reshape(-1)
    choose = (flat_ids[:, None] == jnp.arange(experts, dtype=jnp.int32)[None, :]).astype(jnp.int32)
    earlier = jnp.cumsum(choose, axis=0) - choose
    position = jnp.sum(earlier * choose, axis=1)
    target = flat_ids * capacity + position
    return (target[None, :] == jnp.arange(experts * capacity, dtype=jnp.int32)[:, None]).astype(BF16)


def plain(hidden, weight_rows, expert_ids, gates, cotangent):
    experts = lax.axis_size("expert")
    capacity = hidden.shape[0] // experts
    tok, topk = expert_ids.shape
    width = cotangent.shape[1]
    table = slot_table(expert_ids, experts, capacity)
    weight = lax.all_gather(weight_rows, "dp", axis=0, tiled=True)
    outputs = jnp.dot(hidden, weight, preferred_element_type=F32).astype(BF16)
    back = lax.all_to_all(outputs, "expert", split_axis=0, concat_axis=0, tiled=True)
    picked = lax.dot_general(table, back, (((0,), (0,)), ((), ())), preferred_element_type=F32)
    picked = picked.reshape(tok, topk, width)
    cot32 = cotangent.astype(F32)[:, None, :]
    mixed = jnp.sum(gates[:, :, None] * picked, axis=1).astype(BF16)
    gate_grads = jnp.sum(picked * cot32, axis=2)
    routed = (gates[:, :, None] * cot32).astype(BF16).reshape(-1, width)
    packed = jnp.dot(table, routed, preferred_element_type=F32).astype(BF16)
    grads = lax.all_to_all(packed, "expert", split_axis=0, concat_axis=0, tiled=True)
    hidden_grads = lax.dot_general(
        grads, weight, (((1,), (1,)), ((), ())), preferred_element_type=F32
    ).astype(BF16)
    partial = lax.dot_general(
        hidden, grads, (((0,), (0,)), ((), ())), preferred_element_type=F32
    ).astype(BF16)
    sums = lax.psum_scatter(partial, "dp", scatter_dimension=0, tiled=True)
    return mixed, gate_grads, hidden_grads, sums


def per_device(hidden, w_down, expert_ids, gates, cotangent):
    nd, ne = lax.axis_size("dp"), lax.axis_size("expert")
    rows, width = w_down.shape[1:]
    cap, tok = hidden.shape[0] // ne, expert_ids.shape[0]
    tiled = rows % 16 == 0 and cap % 16 == 0 and tok % 16 == 0 and tok <= 128
    paired = nd == 4 and ne % 2 == 0 and width % 512 == 0
    small = expert_ids.shape[1] <= 8
    body = fused if tiled and paired and small else plain
    mixed, gate_grads, hidden_grads, sums = body(
        hidden, w_down.reshape(rows, width), expert_ids, gates, cotangent
    )
    return mixed, gate_grads, hidden_grads, sums.reshape(1, rows, width)


def solution(mesh):
    split = P(("dp", "expert"), None)
    weights = P("expert", "dp", None)
    return jax.shard_map(
        per_device,
        mesh=mesh,
        in_specs=(split, weights, split, split, split),
        out_specs=(split, split, split, weights),
        check_vma=False,
    )
```

```python
import functools

import jax
import jax.numpy as jnp
from jax import lax
from jax.experimental import pallas as pl
from jax.experimental.pallas import tpu as pltpu
from jax.sharding import PartitionSpec as P

MESH = pl.DeviceIdType.MESH
F32 = jnp.float32
BF16 = jnp.bfloat16


VMEM_BYTES = 67043328


def kernel(
    nd, ne, C, S, A, K, M, groups,
    hidden_in, w, ids_in, gates_in, cot,
    mixed, gate_grads, hidden_grads, weight_grads,
    ids, gates, hidden, wfull, cot_all, cot_far, meta, gg_send, gg_recv,
    ht, gh, ght, ght_far, z, wg_send1, wg_recv1, wg_part, wg_recvp, wg_send2, wg_recv2, wg_own, wg_hold,
    mx_send1, mx_recv1, mx_send2, mx_recv2, mx_own,
    sum_own, sum_send, sum_up, sum_down, sum_send2, sum_recv2,
    wy_r, wf_r, zr, xr, zmr, xmr, cy_r, hy_r, gg_r,
    g1_r, g2_r, m1_r, m2_r, up_r, down_r, sum_r, out_w, out_x, out_g, out_t, out_gg, ready,
):
    N = ne // 2
    rows, D = w.shape
    topk, tok = ids.shape
    F = hidden.shape[1]
    cap = hidden.shape[0] // ne
    T, cw, vw = ne * tok, D // C, D // K
    summed, G = C - S, len(groups)
    lined = sum(last <= M for _, last in groups)
    a, e = lax.axis_index("dp"), lax.axis_index("expert")
    r, c = a // 2, a % 2
    q, x = e // 2, e % 2

    def to(a2, e2):
        return {"dp": a2, "expert": e2}

    pair_e, pair_c, pair_y = to(a, q * 2 + 1 - x), to(r * 2 + 1 - c, e), to((1 - r) * 2 + c, e)
    ahead, behind = to(a, ((q + 1) % N) * 2 + x), to(a, ((q + N - 1) % N) * 2 + x)
    not_last, not_first = q + 1 < N, q > 0
    onward = ((not_last, ahead), (not_first, behind))

    def copy_of(src, dst, ss, rs, dev):
        return pltpu.make_async_remote_copy(
            src_ref=src, dst_ref=dst, send_sem=ss, recv_sem=rs, device_id=dev, device_id_type=MESH
        )

    def start(src, dst, ss, rs, dev):
        copy_of(src, dst, ss, rs, dev).start()

    def arrived(ref, sem):
        copy_of(ref, ref, sem, sem, pair_e).wait_recv()

    def left(ref, sem):
        copy_of(ref, ref, sem, sem, pair_e).wait_send()

    def w_rows(block):
        return pl.ds(pl.multiple_of(block * rows, rows), rows)

    def cols(j, width=cw):
        return slice(j * width, (j + 1) * width)

    barrier = pltpu.get_barrier_semaphore()
    for dev in (pair_y, pair_c, pair_e):
        pl.semaphore_signal(barrier, inc=1, device_id=dev, device_id_type=MESH)
    for exists, dev in onward:

        @pl.when(exists)
        def _():
            pl.semaphore_signal(barrier, inc=1, device_id=dev, device_id_type=MESH)

    own_ids = pltpu.make_async_copy(ids_in, ids, out_t.at[0])
    own_gates = pltpu.make_async_copy(gates_in, gates, out_g.at[0])
    own_ids.start()
    own_gates.start()
    for j in range(K):
        pltpu.make_async_copy(w.at[:, cols(j, vw)], wfull.at[j, w_rows(a)], out_w.at[0]).start()
    for j in range(C):
        pltpu.make_async_copy(cot.at[:, cols(j)], cot_all.at[j, q, x], out_x.at[0]).start()
    own_h = pltpu.make_async_copy(hidden_in, hidden, out_gg.at[0])
    own_h.start()

    meta[q, x] = jnp.zeros(meta.shape[2:], F32)
    gg_send[...] = jnp.zeros_like(gg_send)

    @pl.when(q == 0)
    def _():
        sum_up[:, 0] = jnp.zeros_like(sum_up[:, 0])

    @pl.when(q == N - 1)
    def _():
        sum_down[:, N - 1] = jnp.zeros_like(sum_down[:, N - 1])

    own_ids.wait()
    own_gates.wait()
    idf = ids[...].astype(F32)
    meta[q, x, 0:topk, 0:tok] = idf
    meta[q, x, topk : 2 * topk, 0:tok] = gates[...]

    mine, theirs = w_rows(a), w_rows((1 - r) * 2 + c)
    pltpu.make_async_copy(wfull.at[:, mine], wfull.at[:, mine], out_w.at[0]).wait()
    own_c = cot_all.at[:, q, x]
    pltpu.make_async_copy(own_c, own_c, out_x.at[0]).wait()
    pl.semaphore_wait(barrier, 3 + not_last.astype(jnp.int32) + not_first.astype(jnp.int32))

    def there(side, d):
        return q + d < N if side else q >= d

    def at(side, d):
        return q + d if side else q - d

    def place(side, d):
        return q + d - 1 if side else d - 1

    def place_next(side, d):
        return q - 1 + d if side else d

    def pass_pair(p, side, d):
        ref = cot_far.at[p, at(side, d)]
        start(ref, ref, out_x.at[0], zr.at[C + p, place_next(side, d)], onward[side][1])

    def chunk(i):
        return cot_all.at[i] if i < C else cot_far.at[i - C]

    def pass_cot(i, side, d):
        ref = chunk(i).at[at(side, d), x]
        start(ref, ref, out_x.at[0], zr.at[i, place_next(side, d)], onward[side][1])

    def across(i, zq):
        ref = chunk(i).at[zq, x]
        start(ref, ref, out_x.at[0], xr.at[i], pair_e)

    def tell(d):
        for side in range(2):

            @pl.when(there(side, d - 1) & onward[side][0])
            def _():
                pl.semaphore_signal(
                    ready.at[side, d - 2], inc=1, device_id=onward[side][1], device_id_type=MESH
                )

    def hear(d):
        for side in range(2):

            @pl.when(there(side, d))
            def _():
                pl.semaphore_wait(ready.at[side, d - 2], 1)

    def tiles_cross():
        start(meta.at[q, x], meta.at[q, x], out_t.at[0], xmr.at[0], pair_e)

    def tiles_out():
        arrived(meta.at[q, 1 - x], xmr.at[0])
        for d in order:
            start(meta.at[q], meta.at[q], out_t.at[0], zmr.at[0], to(a, ((q + d) % N) * 2 + x))

    def tiles_in():
        arrived(meta.at[0 : N - 1], zmr.at[0])

    def pair_step(p, d):
        if d == 0:
            arrived(cot_far.at[p, q, 1 - x], xr.at[C + p])
        for side in range(2):

            @pl.when(there(side, d) if d else onward[side][0])
            def _():
                if d:
                    arrived(cot_far.at[p, at(side, d)], zr.at[C + p, place(side, d)])
                if 0 < d < N - 1:

                    @pl.when(onward[side][0])
                    def _():
                        pass_pair(p, side, d)

                if d == 0:
                    pass_pair(p, side, d)

    def begin(i):
        for side in range(2):

            @pl.when(onward[side][0])
            def _():
                pass_cot(i, side, 0)

    def step(i, d):
        for side in range(2):

            @pl.when(there(side, d))
            def _():
                arrived(chunk(i).at[at(side, d), x], zr.at[i, place(side, d)])
                if d < N - 1:

                    @pl.when(onward[side][0])
                    def _():
                        pass_cot(i, side, d)

                if i < C:
                    across(i, at(side, d))

    def begin_far():
        arrived(cot_far.at[:, q, x], cy_r.at[0])
        for s in range(A):
            across(C + s, q)

    def cross_all(i):
        for zq in range(N):
            across(i, zq)

    complete = set()

    def gathered(i):
        if i not in complete:
            complete.add(i)
            arrived(chunk(i).at[:, 1 - x], xr.at[i])

    order = sorted(range(1, N), key=lambda d: min(d, N - d))

    def send_w(k):
        ref = wfull.at[slice(*groups[k]), mine]
        start(ref, ref, out_w.at[0], wy_r.at[k], pair_y)

    def share_w(k):
        ref = wfull.at[slice(*groups[k]), mine]
        start(ref, ref, out_w.at[0], wf_r.at[k], pair_c)

    def forward_w(k):
        ref = wfull.at[slice(*groups[k]), theirs]
        arrived(ref, wy_r.at[k])
        start(ref, ref, out_w.at[0], wf_r.at[k], pair_c)

    def send_far():
        start(
            cot_all.at[summed:C, q, x], cot_far.at[:, q, x], out_x.at[0], cy_r.at[0], pair_y
        )

    def placer(slot_row):
        return (lax.broadcasted_iota(jnp.int32, (cap, tok), 0).astype(F32) == slot_row).astype(BF16)

    eye = lax.broadcasted_iota(jnp.int32, (tok, tok), 0) == lax.broadcasted_iota(jnp.int32, (tok, tok), 1)

    def to_row(col):
        return jnp.sum(jnp.where(eye, col, 0.0), axis=0, keepdims=True)

    def to_col(row):
        return jnp.sum(jnp.where(eye, row, 0.0), axis=1, keepdims=True)

    def routes():
        upper = (
            lax.broadcasted_iota(jnp.int32, (tok, tok), 0) < lax.broadcasted_iota(jnp.int32, (tok, tok), 1)
        ).astype(BF16)
        chosen, weight = [], []
        for b in range(ne):
            tile = meta[b // 2, b % 2]
            hit = tile[0:topk, 0:tok] == e.astype(F32)
            chosen.append(jnp.sum(jnp.where(hit, 1.0, 0.0), axis=0, keepdims=True))
            weight.append(jnp.sum(jnp.where(hit, tile[topk : 2 * topk, 0:tok], 0.0), axis=0, keepdims=True))
        choose = jnp.concatenate(chosen, axis=0)
        position = jnp.dot(choose.astype(BF16), upper, preferred_element_type=F32)
        slots = jnp.where(choose > 0.0, position, -1.0)
        return [slots[b : b + 1, :] for b in range(ne)], weight

    def pick(slot_rows, gate_rows):
        for b in range(ne):
            rows_b = lax.dot_general(
                placer(slot_rows[b]), hidden[b * cap : (b + 1) * cap, :], (((0,), (0,)), ((), ())),
                preferred_element_type=F32,
            )
            ht[b // 2, b % 2] = rows_b.astype(BF16)
            gh[b // 2, b % 2] = (to_col(gate_rows[b]) * rows_b).astype(BF16)
        ght[...] = gh[...].reshape(T, F).astype(F32).T.astype(BF16)

    def send_rows():
        there_rows = pl.ds(pl.multiple_of((1 - r) * 2 * rows, 2 * rows), 2 * rows)
        start(ght.at[there_rows], ght_far, out_g.at[0], hy_r.at[0], pair_y)

    def block_of(j, b):
        return jnp.dot(ght[w_rows(b), :], cot_all[j].reshape(T, cw), preferred_element_type=F32)

    def begin_grads(j):
        gathered(j)
        for k in range(2):
            wg_send1[j, k] = block_of(j, ((r + k) % 2) * 2 + 1 - c).astype(BF16)
        start(wg_send1.at[j], wg_recv1.at[j], out_g.at[0], g1_r.at[j], pair_c)
        wg_hold[j] = block_of(j, (1 - r) * 2 + c)
        wg_own[j] = block_of(j, r * 2 + c)

    def pass_grads(j):
        arrived(wg_recv1.at[j], g1_r.at[j])
        wg_send2[j] = (wg_hold[j] + wg_recv1[j, 1].astype(F32)).astype(BF16)
        start(wg_send2.at[j], wg_recv2.at[j], out_g.at[0], g2_r.at[j], pair_y)

    def full_grads(j):
        s = j - summed
        gathered(j)
        if s >= A:
            gathered(C + s)
        if s == 0:
            arrived(ght_far, hy_r.at[0])

        def both(core):
            other = jnp.dot(
                ght_far[w_rows(core), :], cot_far[s].reshape(T, cw), preferred_element_type=F32
            )
            return block_of(j, r * 2 + core) + other

        wg_part[s] = both(1 - c).astype(BF16)
        start(wg_part.at[s], wg_recvp.at[s], out_g.at[0], g1_r.at[j], pair_c)
        wg_own[j] = both(c)

    def out_part(k):
        piece = slice(*groups[k])
        arrived(wfull.at[piece, 0 : 2 * rows], wf_r.at[k])
        if k < lined:
            for j in range(*groups[k]):
                val = jnp.dot(gh[...].reshape(T, F), wfull[j], preferred_element_type=F32)
                sum_own[j] = val.reshape(N, 2, tok, vw)
                line_step(j, 0)
            return
        lhs = gh[:, pl.ds(1 - x, 1)].reshape(N * tok, F)
        for j in range(*groups[k]):
            val = jnp.dot(lhs, wfull[j], preferred_element_type=F32)
            mx_send1[j] = val.astype(BF16).reshape(N, tok, vw)
        start(mx_send1.at[piece], mx_recv1.at[piece], out_x.at[0], m1_r.at[k - lined], pair_e)
        lhs = gh[:, pl.ds(x, 1)].reshape(N * tok, F)
        for j in range(*groups[k]):
            val = jnp.dot(lhs, wfull[j], preferred_element_type=F32)
            mx_own[j] = val.reshape(N, tok, vw)

    def z_part(k):
        for j in range(*groups[k]):
            i = j * vw // cw
            gathered(i)
            part = cot_all[i, :, :, :, cols(j % (cw // vw), vw)].reshape(T, vw)
            val = lax.dot_general(part, wfull[j], (((1,), (1,)), ((), ())), preferred_element_type=F32)
            z[...] = val if j == 0 else z[...] + val

    def line_step(j, d):
        last = N - 1 - d

        @pl.when(q == d)
        def _():
            if d:
                arrived(sum_up.at[j, d:N], up_r.at[j])
            for o in range(d + 1, N):
                total = sum_own[j, o] + sum_up[j, o].astype(F32) if d else sum_own[j, o]
                sum_send[j, o] = total.astype(BF16)
            if d < N - 1:
                piece = pl.ds(d + 1, N - 1 - d)
                start(sum_send.at[j, piece], sum_up.at[j, piece], out_x.at[0], up_r.at[j], ahead)

        @pl.when(q == last)
        def _():
            if d:
                arrived(sum_down.at[j, 0 : last + 1], down_r.at[j])
            for o in range(last):
                total = sum_own[j, o] + sum_down[j, o].astype(F32) if d else sum_own[j, o]
                sum_send[j, o] = total.astype(BF16)
            if last:
                piece = pl.ds(0, last)
                start(sum_send.at[j, piece], sum_down.at[j, piece], out_x.at[0], down_r.at[j], behind)

    def line_sum(j, xq):
        return sum_own[j, q, xq] + sum_up[j, q, xq].astype(F32) + sum_down[j, q, xq].astype(F32)

    def line_cross(j):
        sum_send2[j] = line_sum(j, 1 - x).astype(BF16)
        start(sum_send2.at[j], sum_recv2.at[j], out_x.at[0], sum_r.at[j], pair_e)

    def finish_line(j):
        arrived(sum_recv2.at[j], sum_r.at[j])
        mixed[:, cols(j, vw)] = (line_sum(j, x) + sum_recv2[j].astype(F32)).astype(BF16)

    early = groups[-2][0]

    def mix_part(k):
        piece = slice(*groups[k])
        arrived(mx_recv1.at[piece], m1_r.at[k - lined])
        sem = m2_r.at[max(0, k - len(groups) + 3)]
        for d in order:
            o = (q + d) % N
            for j in range(*groups[k]):
                mx_send2[j, o] = (mx_own[j, o] + mx_recv1[j, o].astype(F32)).astype(BF16)
            start(mx_send2.at[piece, o], mx_recv2.at[piece, q], out_x.at[0], sem, to(a, o * 2 + x))

    def hidden_part(slot_rows, gate_rows):
        for b in range(ne):
            zb = z[b * tok : (b + 1) * tok, :]
            gg_col = jnp.sum(ht[b // 2, b % 2].astype(F32) * zb, axis=1, keepdims=True)
            gg_send[b, 0:1, 0:tok] = to_row(gg_col)
            scaled = (to_col(gate_rows[b]) * zb).astype(BF16)
            hidden_grads[b * cap : (b + 1) * cap, :] = jnp.dot(
                placer(slot_rows[b]), scaled, preferred_element_type=F32
            ).astype(BF16)
        for d in range(1, ne):
            o = (e + d) % ne
            start(gg_send.at[o], gg_recv.at[e], out_gg.at[0], gg_r.at[0], to(a, o))
        gg_recv[e] = gg_send[e]

    def finish_mixed(k):
        first, last = (M, early) if k == 0 else groups[k - 3]
        arrived(mx_recv2.at[first:last, 0 : N - 1], m2_r.at[k])
        for j in range(first, last):
            total = mx_own[j, q] + mx_recv1[j, q].astype(F32)
            for d in order:
                total = total + mx_recv2[j, (q - d + N) % N].astype(F32)
            mixed[:, cols(j, vw)] = total.astype(BF16)

    def finish_gates():
        arrived(gg_recv.at[0 : ne - 1], gg_r.at[0])
        for k in range(topk):
            row = jnp.zeros((1, tok), F32)
            for b in range(ne):
                row = row + jnp.where(idf[k : k + 1, :] == float(b), gg_recv[b, 0:1, 0:tok], 0.0)
            gate_grads[k : k + 1, :] = row

    def finish_grads(j):
        if j >= summed:
            arrived(wg_recvp.at[j - summed], g1_r.at[j])
            weight_grads[:, cols(j)] = (wg_own[j] + wg_recvp[j - summed].astype(F32)).astype(BF16)
            return
        val = wg_own[j] + wg_recv1[j, 0].astype(F32)
        arrived(wg_recv2.at[j], g2_r.at[j])
        weight_grads[:, cols(j)] = (val + wg_recv2[j].astype(F32)).astype(BF16)

    tiles_cross()
    send_far()
    for k in range(len(groups)):
        send_w(k)
    for j in range(C):
        across(j, q)
    begin(0)
    begin(1)
    begin(2)
    for d in range(2, N):
        tell(d)
        if d == 2:
            for k in range(len(groups)):
                share_w(k)
        hear(d)
    tiles_out()
    begin(3)
    step(0, 1)
    step(1, 1)
    begin_far()
    begin(5)
    step(2, 1)
    step(3, 1)
    step(0, 2)
    forward_w(0)
    step(1, 2)
    pair_step(0, 0)
    own_h.wait()
    tiles_in()
    slot_rows, gate_rows = routes()
    pick(slot_rows, gate_rows)
    send_rows()
    out_part(0)
    step(2, 2)
    step(3, 2)
    step(5, 1)
    step(0, 3)
    forward_w(1)
    step(1, 3)
    out_part(1)
    line_step(0, 1)
    step(2, 3)
    line_step(1, 1)
    step(3, 3)
    step(5, 2)
    pair_step(0, 1)
    forward_w(2)
    forward_w(3)
    out_part(2)
    begin_grads(0)
    line_step(0, 2)
    forward_w(4)
    out_part(3)
    line_step(1, 2)
    pass_grads(0)
    mix_part(1)
    step(5, 3)
    forward_w(5)
    out_part(4)
    begin_grads(1)
    pair_step(0, 2)
    mix_part(2)
    z_part(0)
    out_part(5)
    cross_all(5)
    pass_grads(1)
    z_part(1)
    z_part(2)
    mix_part(3)
    z_part(3)
    z_part(4)
    z_part(5)
    hidden_part(slot_rows, gate_rows)
    line_step(0, 3)
    line_cross(0)
    mix_part(4)
    line_step(1, 3)
    line_cross(1)
    mix_part(5)
    pair_step(0, 3)
    full_grads(2)
    full_grads(3)
    for j in range(M):
        finish_line(j)
    finish_mixed(0)
    finish_gates()
    finish_grads(2)
    finish_grads(0)
    finish_mixed(1)
    finish_grads(1)
    finish_grads(3)
    finish_mixed(2)

    left(wfull.at[:, 0 : 3 * rows], out_w.at[0])
    left(wfull.at[:, 0 : 2 * rows + 2 * rows * T // D], out_g.at[0])
    once = (C * N + A + (S - A) * N + S) * tok // C + (2 * N - 1) * tok
    each = (C + S + A) * tok // C
    for inner in range(2):

        @pl.when((not_first & not_last) if inner else ~(not_first & not_last))
        def _():
            left(wfull.at[:, 0 : once + each * (N + 1 if inner else 1)], out_x.at[0])

    left(gg_recv.at[0 : 2 * N - 1], out_t.at[0])
    left(gg_send.at[0 : ne - 1], out_gg.at[0])


def store_kernel(count, *refs):
    sems = refs[-1]
    copies = [pltpu.make_async_copy(refs[i], refs[count + i], sems.at[i]) for i in range(count)]
    for copy in copies:
        copy.start()
    for copy in copies:
        copy.wait()


def fused(hidden, weight_rows, expert_ids, gates, cotangent):
    nd, ne = lax.axis_size("dp"), lax.axis_size("expert")
    rows, D = weight_rows.shape
    tok, topk = expert_ids.shape
    F = hidden.shape[1]
    T, N = ne * tok, ne // 2
    C, S, A, K, M = 4, 2, 1, 8, 2
    groups = ((0, 2), (2, 4), (4, 5), (5, 6), (6, 7), (7, 8))
    G = len(groups)
    cw, vw, summed = D // C, D // K, C - S
    vm = pltpu.VMEM
    sem = lambda *n: pltpu.SemaphoreType.DMA(tuple(max(i, 1) for i in n))
    near, far = pl.BlockSpec(memory_space=pltpu.VMEM), pl.BlockSpec(memory_space=pltpu.HBM)
    shapes = [((tok, D), BF16), ((topk, tok), F32), (hidden.shape, BF16), ((rows, D), BF16)]
    tall = -(-2 * topk // 8) * 8
    result_bytes = 2 * (tok * D + hidden.size + rows * D) + 128 * 1024
    results = pl.pallas_call(
        functools.partial(kernel, nd, ne, C, S, A, K, M, groups),
        out_shape=tuple(pltpu.VMEM(*s) for s in shapes),
        in_specs=[far] * 5,
        out_specs=(near,) * 4,
        scratch_shapes=[
            vm((topk, tok), jnp.int32), vm((topk, tok), F32), vm(hidden.shape, BF16), vm((K, F, vw), BF16), vm((C, N, 2, tok, cw), BF16),
            vm((S, N, 2, tok, cw), BF16),
            vm((N, 2, tall, 128), F32), vm((ne, 8, 128), F32), vm((ne, 8, 128), F32),
            vm((N, 2, tok, F), BF16), vm((N, 2, tok, F), BF16), vm((F, T), BF16), vm((2 * rows, T), BF16),
            vm((T, F), F32),
            vm((summed, 2, rows, cw), BF16), vm((summed, 2, rows, cw), BF16),
            vm((S, rows, cw), BF16), vm((S, rows, cw), BF16),
            vm((summed, rows, cw), BF16), vm((summed, rows, cw), BF16), vm((C, rows, cw), F32),
            vm((summed, rows, cw), F32),
            vm((K, N, tok, vw), BF16), vm((K, N, tok, vw), BF16),
            vm((K, N, tok, vw), BF16), vm((K, N, tok, vw), BF16), vm((K, N, tok, vw), F32),
            vm((M, N, 2, tok, vw), F32), vm((M, N, 2, tok, vw), BF16), vm((M, N, 2, tok, vw), BF16),
            vm((M, N, 2, tok, vw), BF16), vm((M, tok, vw), BF16), vm((M, tok, vw), BF16),
            sem(G), sem(G), sem(C + S, N - 1), sem(C + S), sem(1), sem(1), sem(1), sem(1), sem(1),
            sem(C), sem(summed), sem(G - sum(last <= M for _, last in groups)), sem(3), sem(M), sem(M), sem(M), sem(1), sem(1), sem(1), sem(1), sem(1),
            pltpu.SemaphoreType.REGULAR((2, max(N - 2, 1))),
        ],
        compiler_params=pltpu.CompilerParams(
            collective_id=0, has_side_effects=True, vmem_limit_bytes=VMEM_BYTES - result_bytes
        ),
    )(hidden, weight_rows, expert_ids.T, gates.T, cotangent)
    mixed, gate_grads, hidden_grads, sums = pl.pallas_call(
        functools.partial(store_kernel, len(shapes)),
        out_shape=tuple(jax.ShapeDtypeStruct(*s) for s in shapes),
        in_specs=[pl.BlockSpec(memory_space=pl.ANY)] * 4,
        out_specs=(far,) * 4,
        scratch_shapes=[sem(len(shapes))],
        compiler_params=pltpu.CompilerParams(vmem_limit_bytes=1024 * 1024),
    )(*results)
    return mixed, gate_grads.T, hidden_grads, sums


def slot_table(expert_ids, experts, capacity):
    flat_ids = expert_ids.reshape(-1)
    choose = (flat_ids[:, None] == jnp.arange(experts, dtype=jnp.int32)[None, :]).astype(jnp.int32)
    earlier = jnp.cumsum(choose, axis=0) - choose
    position = jnp.sum(earlier * choose, axis=1)
    target = flat_ids * capacity + position
    return (target[None, :] == jnp.arange(experts * capacity, dtype=jnp.int32)[:, None]).astype(BF16)


def plain(hidden, weight_rows, expert_ids, gates, cotangent):
    experts = lax.axis_size("expert")
    capacity = hidden.shape[0] // experts
    tok, topk = expert_ids.shape
    width = cotangent.shape[1]
    table = slot_table(expert_ids, experts, capacity)
    weight = lax.all_gather(weight_rows, "dp", axis=0, tiled=True)
    outputs = jnp.dot(hidden, weight, preferred_element_type=F32).astype(BF16)
    back = lax.all_to_all(outputs, "expert", split_axis=0, concat_axis=0, tiled=True)
    picked = lax.dot_general(table, back, (((0,), (0,)), ((), ())), preferred_element_type=F32)
    picked = picked.reshape(tok, topk, width)
    cot32 = cotangent.astype(F32)[:, None, :]
    mixed = jnp.sum(gates[:, :, None] * picked, axis=1).astype(BF16)
    gate_grads = jnp.sum(picked * cot32, axis=2)
    routed = (gates[:, :, None] * cot32).astype(BF16).reshape(-1, width)
    packed = jnp.dot(table, routed, preferred_element_type=F32).astype(BF16)
    grads = lax.all_to_all(packed, "expert", split_axis=0, concat_axis=0, tiled=True)
    hidden_grads = lax.dot_general(
        grads, weight, (((1,), (1,)), ((), ())), preferred_element_type=F32
    ).astype(BF16)
    partial = lax.dot_general(
        hidden, grads, (((0,), (0,)), ((), ())), preferred_element_type=F32
    ).astype(BF16)
    sums = lax.psum_scatter(partial, "dp", scatter_dimension=0, tiled=True)
    return mixed, gate_grads, hidden_grads, sums


def per_device(hidden, w_down, expert_ids, gates, cotangent):
    nd, ne = lax.axis_size("dp"), lax.axis_size("expert")
    rows, width = w_down.shape[1:]
    cap, tok = hidden.shape[0] // ne, expert_ids.shape[0]
    tiled = rows % 16 == 0 and cap % 16 == 0 and tok % 16 == 0 and tok <= 128
    paired = nd == 4 and ne % 2 == 0 and width % 512 == 0
    small = expert_ids.shape[1] <= 8
    body = fused if tiled and paired and small else plain
    mixed, gate_grads, hidden_grads, sums = body(
        hidden, w_down.reshape(rows, width), expert_ids, gates, cotangent
    )
    return mixed, gate_grads, hidden_grads, sums.reshape(1, rows, width)


def solution(mesh):
    split = P(("dp", "expert"), None)
    weights = P("expert", "dp", None)
    return jax.shard_map(
        per_device,
        mesh=mesh,
        in_specs=(split, weights, split, split, split),
        out_specs=(split, split, split, weights),
        check_vma=False,
    )
```

```python
import functools

import jax
import jax.numpy as jnp
from jax import lax
from jax.experimental import pallas as pl
from jax.experimental.pallas import tpu as pltpu
from jax.sharding import PartitionSpec as P

MESH = pl.DeviceIdType.MESH
F32 = jnp.float32
BF16 = jnp.bfloat16


VMEM_BYTES = 67043328


def kernel(
    nd, ne, C, S, A, K, M, groups,
    hidden_in, w, ids_in, gates_in, cot,
    mixed, gate_grads, hidden_grads, weight_grads,
    ids, gates, hidden, wfull, cot_all, cot_far, meta, gg_send, gg_recv,
    ht, gh, ght, ght_far, z, wg_send1, wg_recv1, wg_part, wg_recvp, wg_send2, wg_recv2, wg_own, wg_hold,
    mx_send1, mx_recv1, mx_send2, mx_recv2, mx_own,
    sum_own, sum_send, sum_up, sum_down, sum_send2, sum_recv2,
    wy_r, wf_r, zr, xr, zmr, xmr, cy_r, hy_r, gg_r,
    g1_r, g2_r, m1_r, m2_r, up_r, down_r, sum_r, out_w, out_x, out_g, out_t, out_gg, ready,
):
    N = ne // 2
    rows, D = w.shape
    topk, tok = ids.shape
    F = hidden.shape[1]
    cap = hidden.shape[0] // ne
    T, cw, vw = ne * tok, D // C, D // K
    summed, G = C - S, len(groups)
    lined = sum(last <= M for _, last in groups)
    a, e = lax.axis_index("dp"), lax.axis_index("expert")
    r, c = a // 2, a % 2
    q, x = e // 2, e % 2

    def to(a2, e2):
        return {"dp": a2, "expert": e2}

    pair_e, pair_c, pair_y = to(a, q * 2 + 1 - x), to(r * 2 + 1 - c, e), to((1 - r) * 2 + c, e)
    ahead, behind = to(a, ((q + 1) % N) * 2 + x), to(a, ((q + N - 1) % N) * 2 + x)
    not_last, not_first = q + 1 < N, q > 0
    onward = ((not_last, ahead), (not_first, behind))

    def copy_of(src, dst, ss, rs, dev):
        return pltpu.make_async_remote_copy(
            src_ref=src, dst_ref=dst, send_sem=ss, recv_sem=rs, device_id=dev, device_id_type=MESH
        )

    def start(src, dst, ss, rs, dev):
        copy_of(src, dst, ss, rs, dev).start()

    def arrived(ref, sem):
        copy_of(ref, ref, sem, sem, pair_e).wait_recv()

    def left(ref, sem):
        copy_of(ref, ref, sem, sem, pair_e).wait_send()

    def w_rows(block):
        return pl.ds(pl.multiple_of(block * rows, rows), rows)

    def cols(j, width=cw):
        return slice(j * width, (j + 1) * width)

    barrier = pltpu.get_barrier_semaphore()
    for dev in (pair_y, pair_c, pair_e):
        pl.semaphore_signal(barrier, inc=1, device_id=dev, device_id_type=MESH)
    for exists, dev in onward:

        @pl.when(exists)
        def _():
            pl.semaphore_signal(barrier, inc=1, device_id=dev, device_id_type=MESH)

    own_ids = pltpu.make_async_copy(ids_in, ids, out_t.at[0])
    own_gates = pltpu.make_async_copy(gates_in, gates, out_g.at[0])
    own_ids.start()
    own_gates.start()
    for j in range(K):
        pltpu.make_async_copy(w.at[:, cols(j, vw)], wfull.at[j, w_rows(a)], out_w.at[0]).start()
    for j in range(C):
        pltpu.make_async_copy(cot.at[:, cols(j)], cot_all.at[j, q, x], out_x.at[0]).start()
    own_h = pltpu.make_async_copy(hidden_in, hidden, out_gg.at[0])
    own_h.start()

    meta[q, x] = jnp.zeros(meta.shape[2:], F32)
    gg_send[...] = jnp.zeros_like(gg_send)

    @pl.when(q == 0)
    def _():
        sum_up[:, 0] = jnp.zeros_like(sum_up[:, 0])

    @pl.when(q == N - 1)
    def _():
        sum_down[:, N - 1] = jnp.zeros_like(sum_down[:, N - 1])

    own_ids.wait()
    own_gates.wait()
    idf = ids[...].astype(F32)
    meta[q, x, 0:topk, 0:tok] = idf
    meta[q, x, topk : 2 * topk, 0:tok] = gates[...]

    mine, theirs = w_rows(a), w_rows((1 - r) * 2 + c)
    pltpu.make_async_copy(wfull.at[:, mine], wfull.at[:, mine], out_w.at[0]).wait()
    own_c = cot_all.at[:, q, x]
    pltpu.make_async_copy(own_c, own_c, out_x.at[0]).wait()
    pl.semaphore_wait(barrier, 3 + not_last.astype(jnp.int32) + not_first.astype(jnp.int32))

    def there(side, d):
        return q + d < N if side else q >= d

    def at(side, d):
        return q + d if side else q - d

    def place(side, d):
        return q + d - 1 if side else d - 1

    def place_next(side, d):
        return q - 1 + d if side else d

    def pass_pair(p, side, d):
        ref = cot_far.at[p, at(side, d)]
        start(ref, ref, out_x.at[0], zr.at[C + p, place_next(side, d)], onward[side][1])

    def chunk(i):
        return cot_all.at[i] if i < C else cot_far.at[i - C]

    def pass_cot(i, side, d):
        ref = chunk(i).at[at(side, d), x]
        start(ref, ref, out_x.at[0], zr.at[i, place_next(side, d)], onward[side][1])

    def across(i, zq):
        ref = chunk(i).at[zq, x]
        start(ref, ref, out_x.at[0], xr.at[i], pair_e)

    def tell(d):
        for side in range(2):

            @pl.when(there(side, d - 1) & onward[side][0])
            def _():
                pl.semaphore_signal(
                    ready.at[side, d - 2], inc=1, device_id=onward[side][1], device_id_type=MESH
                )

    def hear(d):
        for side in range(2):

            @pl.when(there(side, d))
            def _():
                pl.semaphore_wait(ready.at[side, d - 2], 1)

    def tiles_cross():
        start(meta.at[q, x], meta.at[q, x], out_t.at[0], xmr.at[0], pair_e)

    def tiles_out():
        arrived(meta.at[q, 1 - x], xmr.at[0])
        for d in order:
            start(meta.at[q], meta.at[q], out_t.at[0], zmr.at[0], to(a, ((q + d) % N) * 2 + x))

    def tiles_in():
        arrived(meta.at[0 : N - 1], zmr.at[0])

    def pair_step(p, d):
        if d == 0:
            arrived(cot_far.at[p, q, 1 - x], xr.at[C + p])
        for side in range(2):

            @pl.when(there(side, d) if d else onward[side][0])
            def _():
                if d:
                    arrived(cot_far.at[p, at(side, d)], zr.at[C + p, place(side, d)])
                if 0 < d < N - 1:

                    @pl.when(onward[side][0])
                    def _():
                        pass_pair(p, side, d)

                if d == 0:
                    pass_pair(p, side, d)

    def begin(i):
        for side in range(2):

            @pl.when(onward[side][0])
            def _():
                pass_cot(i, side, 0)

    def step(i, d):
        for side in range(2):

            @pl.when(there(side, d))
            def _():
                arrived(chunk(i).at[at(side, d), x], zr.at[i, place(side, d)])
                if d < N - 1:

                    @pl.when(onward[side][0])
                    def _():
                        pass_cot(i, side, d)

                if i < C:
                    across(i, at(side, d))

    def begin_far():
        arrived(cot_far.at[:, q, x], cy_r.at[0])
        for s in range(A):
            across(C + s, q)

    def cross_all(i):
        for zq in range(N):
            across(i, zq)

    complete = set()

    def gathered(i):
        if i not in complete:
            complete.add(i)
            arrived(chunk(i).at[:, 1 - x], xr.at[i])

    order = sorted(range(1, N), key=lambda d: min(d, N - d))

    def send_w(k):
        ref = wfull.at[slice(*groups[k]), mine]
        start(ref, ref, out_w.at[0], wy_r.at[k], pair_y)

    def share_w(k):
        ref = wfull.at[slice(*groups[k]), mine]
        start(ref, ref, out_w.at[0], wf_r.at[k], pair_c)

    def forward_w(k):
        ref = wfull.at[slice(*groups[k]), theirs]
        arrived(ref, wy_r.at[k])
        start(ref, ref, out_w.at[0], wf_r.at[k], pair_c)

    def send_far():
        start(
            cot_all.at[summed:C, q, x], cot_far.at[:, q, x], out_x.at[0], cy_r.at[0], pair_y
        )

    def placer(slot_row):
        return (lax.broadcasted_iota(jnp.int32, (cap, tok), 0).astype(F32) == slot_row).astype(BF16)

    eye = lax.broadcasted_iota(jnp.int32, (tok, tok), 0) == lax.broadcasted_iota(jnp.int32, (tok, tok), 1)

    def to_row(col):
        return jnp.sum(jnp.where(eye, col, 0.0), axis=0, keepdims=True)

    def to_col(row):
        return jnp.sum(jnp.where(eye, row, 0.0), axis=1, keepdims=True)

    def routes():
        upper = (
            lax.broadcasted_iota(jnp.int32, (tok, tok), 0) < lax.broadcasted_iota(jnp.int32, (tok, tok), 1)
        ).astype(BF16)
        chosen, weight = [], []
        for b in range(ne):
            tile = meta[b // 2, b % 2]
            hit = tile[0:topk, 0:tok] == e.astype(F32)
            chosen.append(jnp.sum(jnp.where(hit, 1.0, 0.0), axis=0, keepdims=True))
            weight.append(jnp.sum(jnp.where(hit, tile[topk : 2 * topk, 0:tok], 0.0), axis=0, keepdims=True))
        choose = jnp.concatenate(chosen, axis=0)
        position = jnp.dot(choose.astype(BF16), upper, preferred_element_type=F32)
        slots = jnp.where(choose > 0.0, position, -1.0)
        return [slots[b : b + 1, :] for b in range(ne)], weight

    def pick(slot_rows, gate_rows):
        for b in range(ne):
            rows_b = lax.dot_general(
                placer(slot_rows[b]), hidden[b * cap : (b + 1) * cap, :], (((0,), (0,)), ((), ())),
                preferred_element_type=F32,
            )
            ht[b // 2, b % 2] = rows_b.astype(BF16)
            gh[b // 2, b % 2] = (to_col(gate_rows[b]) * rows_b).astype(BF16)
        ght[...] = gh[...].reshape(T, F).astype(F32).T.astype(BF16)

    def send_rows():
        there_rows = pl.ds(pl.multiple_of((1 - r) * 2 * rows, 2 * rows), 2 * rows)
        start(ght.at[there_rows], ght_far, out_g.at[0], hy_r.at[0], pair_y)

    def block_of(j, b):
        return jnp.dot(ght[w_rows(b), :], cot_all[j].reshape(T, cw), preferred_element_type=F32)

    def begin_grads(j):
        gathered(j)
        for k in range(2):
            wg_send1[j, k] = block_of(j, ((r + k) % 2) * 2 + 1 - c).astype(BF16)
        start(wg_send1.at[j], wg_recv1.at[j], out_g.at[0], g1_r.at[j], pair_c)
        wg_hold[j] = block_of(j, (1 - r) * 2 + c)
        wg_own[j] = block_of(j, r * 2 + c)

    def pass_grads(j):
        arrived(wg_recv1.at[j], g1_r.at[j])
        wg_send2[j] = (wg_hold[j] + wg_recv1[j, 1].astype(F32)).astype(BF16)
        start(wg_send2.at[j], wg_recv2.at[j], out_g.at[0], g2_r.at[j], pair_y)

    def full_grads(j):
        s = j - summed
        gathered(j)
        if s >= A:
            gathered(C + s)
        if s == 0:
            arrived(ght_far, hy_r.at[0])

        def both(core):
            other = jnp.dot(
                ght_far[w_rows(core), :], cot_far[s].reshape(T, cw), preferred_element_type=F32
            )
            return block_of(j, r * 2 + core) + other

        wg_part[s] = both(1 - c).astype(BF16)
        start(wg_part.at[s], wg_recvp.at[s], out_g.at[0], g1_r.at[j], pair_c)
        wg_own[j] = both(c)

    def out_part(k):
        piece = slice(*groups[k])
        arrived(wfull.at[piece, 0 : 2 * rows], wf_r.at[k])
        if k < lined:
            for j in range(*groups[k]):
                val = jnp.dot(gh[...].reshape(T, F), wfull[j], preferred_element_type=F32)
                sum_own[j] = val.reshape(N, 2, tok, vw)
                line_step(j, 0)
            return
        lhs = gh[:, pl.ds(1 - x, 1)].reshape(N * tok, F)
        for j in range(*groups[k]):
            val = jnp.dot(lhs, wfull[j], preferred_element_type=F32)
            mx_send1[j] = val.astype(BF16).reshape(N, tok, vw)
        start(mx_send1.at[piece], mx_recv1.at[piece], out_x.at[0], m1_r.at[k - lined], pair_e)
        lhs = gh[:, pl.ds(x, 1)].reshape(N * tok, F)
        for j in range(*groups[k]):
            val = jnp.dot(lhs, wfull[j], preferred_element_type=F32)
            mx_own[j] = val.reshape(N, tok, vw)

    def z_part(k):
        for j in range(*groups[k]):
            i = j * vw // cw
            gathered(i)
            part = cot_all[i, :, :, :, cols(j % (cw // vw), vw)].reshape(T, vw)
            val = lax.dot_general(part, wfull[j], (((1,), (1,)), ((), ())), preferred_element_type=F32)
            z[...] = val if j == 0 else z[...] + val

    def line_step(j, d):
        last = N - 1 - d

        @pl.when(q == d)
        def _():
            if d:
                arrived(sum_up.at[j, d:N], up_r.at[j])
            for o in range(d + 1, N):
                total = sum_own[j, o] + sum_up[j, o].astype(F32) if d else sum_own[j, o]
                sum_send[j, o] = total.astype(BF16)
            if d < N - 1:
                piece = pl.ds(d + 1, N - 1 - d)
                start(sum_send.at[j, piece], sum_up.at[j, piece], out_x.at[0], up_r.at[j], ahead)

        @pl.when(q == last)
        def _():
            if d:
                arrived(sum_down.at[j, 0 : last + 1], down_r.at[j])
            for o in range(last):
                total = sum_own[j, o] + sum_down[j, o].astype(F32) if d else sum_own[j, o]
                sum_send[j, o] = total.astype(BF16)
            if last:
                piece = pl.ds(0, last)
                start(sum_send.at[j, piece], sum_down.at[j, piece], out_x.at[0], down_r.at[j], behind)

    def line_sum(j, xq):
        return sum_own[j, q, xq] + sum_up[j, q, xq].astype(F32) + sum_down[j, q, xq].astype(F32)

    def line_cross(j):
        sum_send2[j] = line_sum(j, 1 - x).astype(BF16)
        start(sum_send2.at[j], sum_recv2.at[j], out_x.at[0], sum_r.at[j], pair_e)

    def finish_line(j):
        arrived(sum_recv2.at[j], sum_r.at[j])
        mixed[:, cols(j, vw)] = (line_sum(j, x) + sum_recv2[j].astype(F32)).astype(BF16)

    early = groups[-2][0]

    def mix_part(k):
        piece = slice(*groups[k])
        arrived(mx_recv1.at[piece], m1_r.at[k - lined])
        sem = m2_r.at[max(0, k - len(groups) + 3)]
        for d in order:
            o = (q + d) % N
            for j in range(*groups[k]):
                mx_send2[j, o] = (mx_own[j, o] + mx_recv1[j, o].astype(F32)).astype(BF16)
            start(mx_send2.at[piece, o], mx_recv2.at[piece, q], out_x.at[0], sem, to(a, o * 2 + x))

    def hidden_part(slot_rows, gate_rows):
        for b in range(ne):
            zb = z[b * tok : (b + 1) * tok, :]
            gg_col = jnp.sum(ht[b // 2, b % 2].astype(F32) * zb, axis=1, keepdims=True)
            gg_send[b, 0:1, 0:tok] = to_row(gg_col)
            scaled = (to_col(gate_rows[b]) * zb).astype(BF16)
            hidden_grads[b * cap : (b + 1) * cap, :] = jnp.dot(
                placer(slot_rows[b]), scaled, preferred_element_type=F32
            ).astype(BF16)
        for d in range(1, ne):
            o = (e + d) % ne
            start(gg_send.at[o], gg_recv.at[e], out_gg.at[0], gg_r.at[0], to(a, o))
        gg_recv[e] = gg_send[e]

    def finish_mixed(k):
        first, last = (M, early) if k == 0 else groups[k - 3]
        arrived(mx_recv2.at[first:last, 0 : N - 1], m2_r.at[k])
        for j in range(first, last):
            total = mx_own[j, q] + mx_recv1[j, q].astype(F32)
            for d in order:
                total = total + mx_recv2[j, (q - d + N) % N].astype(F32)
            mixed[:, cols(j, vw)] = total.astype(BF16)

    def finish_gates():
        arrived(gg_recv.at[0 : ne - 1], gg_r.at[0])
        for k in range(topk):
            row = jnp.zeros((1, tok), F32)
            for b in range(ne):
                row = row + jnp.where(idf[k : k + 1, :] == float(b), gg_recv[b, 0:1, 0:tok], 0.0)
            gate_grads[k : k + 1, :] = row

    def finish_grads(j):
        if j >= summed:
            arrived(wg_recvp.at[j - summed], g1_r.at[j])
            weight_grads[:, cols(j)] = (wg_own[j] + wg_recvp[j - summed].astype(F32)).astype(BF16)
            return
        val = wg_own[j] + wg_recv1[j, 0].astype(F32)
        arrived(wg_recv2.at[j], g2_r.at[j])
        weight_grads[:, cols(j)] = (val + wg_recv2[j].astype(F32)).astype(BF16)

    tiles_cross()
    send_far()
    for k in range(len(groups)):
        send_w(k)
    for j in range(C):
        across(j, q)
    begin(0)
    begin(1)
    begin(2)
    for d in range(2, N):
        tell(d)
        if d == 2:
            for k in range(len(groups)):
                share_w(k)
        hear(d)
    tiles_out()
    begin(3)
    step(0, 1)
    step(1, 1)
    begin_far()
    begin(5)
    step(2, 1)
    step(3, 1)
    pair_step(0, 0)
    step(0, 2)
    forward_w(0)
    step(1, 2)
    own_h.wait()
    tiles_in()
    slot_rows, gate_rows = routes()
    pick(slot_rows, gate_rows)
    send_rows()
    out_part(0)
    step(2, 2)
    step(3, 2)
    step(5, 1)
    step(0, 3)
    step(1, 3)
    forward_w(1)
    out_part(1)
    line_step(0, 1)
    step(2, 3)
    line_step(1, 1)
    step(3, 3)
    pair_step(0, 1)
    forward_w(2)
    step(5, 2)
    out_part(2)
    forward_w(3)
    begin_grads(0)
    line_step(0, 2)
    forward_w(4)
    out_part(3)
    line_step(1, 2)
    pass_grads(0)
    mix_part(1)
    step(5, 3)
    forward_w(5)
    out_part(4)
    begin_grads(1)
    pair_step(0, 2)
    mix_part(2)
    z_part(0)
    out_part(5)
    cross_all(5)
    pass_grads(1)
    mix_part(3)
    z_part(1)
    z_part(2)
    z_part(3)
    z_part(4)
    z_part(5)
    hidden_part(slot_rows, gate_rows)
    line_step(0, 3)
    line_cross(0)
    mix_part(4)
    line_step(1, 3)
    line_cross(1)
    mix_part(5)
    pair_step(0, 3)
    full_grads(2)
    full_grads(3)
    for j in range(M):
        finish_line(j)
    finish_mixed(0)
    finish_gates()
    finish_grads(2)
    finish_grads(0)
    finish_mixed(1)
    finish_grads(1)
    finish_grads(3)
    finish_mixed(2)

    left(wfull.at[:, 0 : 3 * rows], out_w.at[0])
    left(wfull.at[:, 0 : 2 * rows + 2 * rows * T // D], out_g.at[0])
    once = (C * N + A + (S - A) * N + S) * tok // C + (2 * N - 1) * tok
    each = (C + S + A) * tok // C
    for inner in range(2):

        @pl.when((not_first & not_last) if inner else ~(not_first & not_last))
        def _():
            left(wfull.at[:, 0 : once + each * (N + 1 if inner else 1)], out_x.at[0])

    left(gg_recv.at[0 : 2 * N - 1], out_t.at[0])
    left(gg_send.at[0 : ne - 1], out_gg.at[0])


def store_kernel(count, *refs):
    sems = refs[-1]
    copies = [pltpu.make_async_copy(refs[i], refs[count + i], sems.at[i]) for i in range(count)]
    for copy in copies:
        copy.start()
    for copy in copies:
        copy.wait()


def fused(hidden, weight_rows, expert_ids, gates, cotangent):
    nd, ne = lax.axis_size("dp"), lax.axis_size("expert")
    rows, D = weight_rows.shape
    tok, topk = expert_ids.shape
    F = hidden.shape[1]
    T, N = ne * tok, ne // 2
    C, S, A, K, M = 4, 2, 1, 8, 2
    groups = ((0, 2), (2, 4), (4, 5), (5, 6), (6, 7), (7, 8))
    G = len(groups)
    cw, vw, summed = D // C, D // K, C - S
    vm = pltpu.VMEM
    sem = lambda *n: pltpu.SemaphoreType.DMA(tuple(max(i, 1) for i in n))
    near, far = pl.BlockSpec(memory_space=pltpu.VMEM), pl.BlockSpec(memory_space=pltpu.HBM)
    shapes = [((tok, D), BF16), ((topk, tok), F32), (hidden.shape, BF16), ((rows, D), BF16)]
    tall = -(-2 * topk // 8) * 8
    result_bytes = 2 * (tok * D + hidden.size + rows * D) + 128 * 1024
    results = pl.pallas_call(
        functools.partial(kernel, nd, ne, C, S, A, K, M, groups),
        out_shape=tuple(pltpu.VMEM(*s) for s in shapes),
        in_specs=[far] * 5,
        out_specs=(near,) * 4,
        scratch_shapes=[
            vm((topk, tok), jnp.int32), vm((topk, tok), F32), vm(hidden.shape, BF16), vm((K, F, vw), BF16), vm((C, N, 2, tok, cw), BF16),
            vm((S, N, 2, tok, cw), BF16),
            vm((N, 2, tall, 128), F32), vm((ne, 8, 128), F32), vm((ne, 8, 128), F32),
            vm((N, 2, tok, F), BF16), vm((N, 2, tok, F), BF16), vm((F, T), BF16), vm((2 * rows, T), BF16),
            vm((T, F), F32),
            vm((summed, 2, rows, cw), BF16), vm((summed, 2, rows, cw), BF16),
            vm((S, rows, cw), BF16), vm((S, rows, cw), BF16),
            vm((summed, rows, cw), BF16), vm((summed, rows, cw), BF16), vm((C, rows, cw), F32),
            vm((summed, rows, cw), F32),
            vm((K, N, tok, vw), BF16), vm((K, N, tok, vw), BF16),
            vm((K, N, tok, vw), BF16), vm((K, N, tok, vw), BF16), vm((K, N, tok, vw), F32),
            vm((M, N, 2, tok, vw), F32), vm((M, N, 2, tok, vw), BF16), vm((M, N, 2, tok, vw), BF16),
            vm((M, N, 2, tok, vw), BF16), vm((M, tok, vw), BF16), vm((M, tok, vw), BF16),
            sem(G), sem(G), sem(C + S, N - 1), sem(C + S), sem(1), sem(1), sem(1), sem(1), sem(1),
            sem(C), sem(summed), sem(G - sum(last <= M for _, last in groups)), sem(3), sem(M), sem(M), sem(M), sem(1), sem(1), sem(1), sem(1), sem(1),
            pltpu.SemaphoreType.REGULAR((2, max(N - 2, 1))),
        ],
        compiler_params=pltpu.CompilerParams(
            collective_id=0, has_side_effects=True, vmem_limit_bytes=VMEM_BYTES - result_bytes
        ),
    )(hidden, weight_rows, expert_ids.T, gates.T, cotangent)
    mixed, gate_grads, hidden_grads, sums = pl.pallas_call(
        functools.partial(store_kernel, len(shapes)),
        out_shape=tuple(jax.ShapeDtypeStruct(*s) for s in shapes),
        in_specs=[pl.BlockSpec(memory_space=pl.ANY)] * 4,
        out_specs=(far,) * 4,
        scratch_shapes=[sem(len(shapes))],
        compiler_params=pltpu.CompilerParams(vmem_limit_bytes=1024 * 1024),
    )(*results)
    return mixed, gate_grads.T, hidden_grads, sums


def slot_table(expert_ids, experts, capacity):
    flat_ids = expert_ids.reshape(-1)
    choose = (flat_ids[:, None] == jnp.arange(experts, dtype=jnp.int32)[None, :]).astype(jnp.int32)
    earlier = jnp.cumsum(choose, axis=0) - choose
    position = jnp.sum(earlier * choose, axis=1)
    target = flat_ids * capacity + position
    return (target[None, :] == jnp.arange(experts * capacity, dtype=jnp.int32)[:, None]).astype(BF16)


def plain(hidden, weight_rows, expert_ids, gates, cotangent):
    experts = lax.axis_size("expert")
    capacity = hidden.shape[0] // experts
    tok, topk = expert_ids.shape
    width = cotangent.shape[1]
    table = slot_table(expert_ids, experts, capacity)
    weight = lax.all_gather(weight_rows, "dp", axis=0, tiled=True)
    outputs = jnp.dot(hidden, weight, preferred_element_type=F32).astype(BF16)
    back = lax.all_to_all(outputs, "expert", split_axis=0, concat_axis=0, tiled=True)
    picked = lax.dot_general(table, back, (((0,), (0,)), ((), ())), preferred_element_type=F32)
    picked = picked.reshape(tok, topk, width)
    cot32 = cotangent.astype(F32)[:, None, :]
    mixed = jnp.sum(gates[:, :, None] * picked, axis=1).astype(BF16)
    gate_grads = jnp.sum(picked * cot32, axis=2)
    routed = (gates[:, :, None] * cot32).astype(BF16).reshape(-1, width)
    packed = jnp.dot(table, routed, preferred_element_type=F32).astype(BF16)
    grads = lax.all_to_all(packed, "expert", split_axis=0, concat_axis=0, tiled=True)
    hidden_grads = lax.dot_general(
        grads, weight, (((1,), (1,)), ((), ())), preferred_element_type=F32
    ).astype(BF16)
    partial = lax.dot_general(
        hidden, grads, (((0,), (0,)), ((), ())), preferred_element_type=F32
    ).astype(BF16)
    sums = lax.psum_scatter(partial, "dp", scatter_dimension=0, tiled=True)
    return mixed, gate_grads, hidden_grads, sums


def per_device(hidden, w_down, expert_ids, gates, cotangent):
    nd, ne = lax.axis_size("dp"), lax.axis_size("expert")
    rows, width = w_down.shape[1:]
    cap, tok = hidden.shape[0] // ne, expert_ids.shape[0]
    tiled = rows % 16 == 0 and cap % 16 == 0 and tok % 16 == 0 and tok <= 128
    paired = nd == 4 and ne % 2 == 0 and width % 512 == 0
    small = expert_ids.shape[1] <= 8
    body = fused if tiled and paired and small else plain
    mixed, gate_grads, hidden_grads, sums = body(
        hidden, w_down.reshape(rows, width), expert_ids, gates, cotangent
    )
    return mixed, gate_grads, hidden_grads, sums.reshape(1, rows, width)


def solution(mesh):
    split = P(("dp", "expert"), None)
    weights = P("expert", "dp", None)
    return jax.shard_map(
        per_device,
        mesh=mesh,
        in_specs=(split, weights, split, split, split),
        out_specs=(split, split, split, weights),
        check_vma=False,
    )
```

```python
import functools

import jax
import jax.numpy as jnp
from jax import lax
from jax.experimental import pallas as pl
from jax.experimental.pallas import tpu as pltpu
from jax.sharding import PartitionSpec as P

MESH = pl.DeviceIdType.MESH
F32 = jnp.float32
BF16 = jnp.bfloat16


VMEM_BYTES = 67043328


def kernel(
    nd, ne, C, S, A, K, M, groups,
    hidden_in, w, ids_in, gates_in, cot,
    mixed, gate_grads, hidden_grads, weight_grads,
    ids, gates, hidden, wfull, cot_all, cot_far, meta, gg_send, gg_recv,
    ht, gh, ght, ght_far, z, wg_send1, wg_recv1, wg_part, wg_recvp, wg_send2, wg_recv2, wg_own, wg_hold,
    mx_send1, mx_recv1, mx_send2, mx_recv2, mx_own,
    sum_own, sum_send, sum_up, sum_down, sum_send2, sum_recv2,
    wy_r, wf_r, zr, xr, zmr, xmr, cy_r, hy_r, gg_r,
    g1_r, g2_r, m1_r, m2_r, up_r, down_r, sum_r, out_w, out_x, out_g, out_t, out_gg, ready,
):
    N = ne // 2
    rows, D = w.shape
    topk, tok = ids.shape
    F = hidden.shape[1]
    cap = hidden.shape[0] // ne
    T, cw, vw = ne * tok, D // C, D // K
    summed, G = C - S, len(groups)
    lined = sum(last <= M for _, last in groups)
    a, e = lax.axis_index("dp"), lax.axis_index("expert")
    r, c = a // 2, a % 2
    q, x = e // 2, e % 2

    def to(a2, e2):
        return {"dp": a2, "expert": e2}

    pair_e, pair_c, pair_y = to(a, q * 2 + 1 - x), to(r * 2 + 1 - c, e), to((1 - r) * 2 + c, e)
    ahead, behind = to(a, ((q + 1) % N) * 2 + x), to(a, ((q + N - 1) % N) * 2 + x)
    not_last, not_first = q + 1 < N, q > 0
    onward = ((not_last, ahead), (not_first, behind))

    def copy_of(src, dst, ss, rs, dev):
        return pltpu.make_async_remote_copy(
            src_ref=src, dst_ref=dst, send_sem=ss, recv_sem=rs, device_id=dev, device_id_type=MESH
        )

    def start(src, dst, ss, rs, dev):
        copy_of(src, dst, ss, rs, dev).start()

    def arrived(ref, sem):
        copy_of(ref, ref, sem, sem, pair_e).wait_recv()

    def left(ref, sem):
        copy_of(ref, ref, sem, sem, pair_e).wait_send()

    def w_rows(block):
        return pl.ds(pl.multiple_of(block * rows, rows), rows)

    def cols(j, width=cw):
        return slice(j * width, (j + 1) * width)

    barrier = pltpu.get_barrier_semaphore()
    for dev in (pair_y, pair_c, pair_e):
        pl.semaphore_signal(barrier, inc=1, device_id=dev, device_id_type=MESH)
    for exists, dev in onward:

        @pl.when(exists)
        def _():
            pl.semaphore_signal(barrier, inc=1, device_id=dev, device_id_type=MESH)

    own_ids = pltpu.make_async_copy(ids_in, ids, out_t.at[0])
    own_gates = pltpu.make_async_copy(gates_in, gates, out_g.at[0])
    own_ids.start()
    own_gates.start()
    for j in range(K):
        pltpu.make_async_copy(w.at[:, cols(j, vw)], wfull.at[j, w_rows(a)], out_w.at[0]).start()
    for j in range(C):
        pltpu.make_async_copy(cot.at[:, cols(j)], cot_all.at[j, q, x], out_x.at[0]).start()
    own_h = pltpu.make_async_copy(hidden_in, hidden, out_gg.at[0])
    own_h.start()

    meta[q, x] = jnp.zeros(meta.shape[2:], F32)
    gg_send[...] = jnp.zeros_like(gg_send)

    @pl.when(q == 0)
    def _():
        sum_up[:, 0] = jnp.zeros_like(sum_up[:, 0])

    @pl.when(q == N - 1)
    def _():
        sum_down[:, N - 1] = jnp.zeros_like(sum_down[:, N - 1])

    own_ids.wait()
    own_gates.wait()
    idf = ids[...].astype(F32)
    meta[q, x, 0:topk, 0:tok] = idf
    meta[q, x, topk : 2 * topk, 0:tok] = gates[...]

    mine, theirs = w_rows(a), w_rows((1 - r) * 2 + c)
    pltpu.make_async_copy(wfull.at[:, mine], wfull.at[:, mine], out_w.at[0]).wait()
    own_c = cot_all.at[:, q, x]
    pltpu.make_async_copy(own_c, own_c, out_x.at[0]).wait()
    pl.semaphore_wait(barrier, 3 + not_last.astype(jnp.int32) + not_first.astype(jnp.int32))

    def there(side, d):
        return q + d < N if side else q >= d

    def at(side, d):
        return q + d if side else q - d

    def place(side, d):
        return q + d - 1 if side else d - 1

    def place_next(side, d):
        return q - 1 + d if side else d

    def pass_pair(p, side, d):
        ref = cot_far.at[p, at(side, d)]
        start(ref, ref, out_x.at[0], zr.at[C + p, place_next(side, d)], onward[side][1])

    def chunk(i):
        return cot_all.at[i] if i < C else cot_far.at[i - C]

    def pass_cot(i, side, d):
        ref = chunk(i).at[at(side, d), x]
        start(ref, ref, out_x.at[0], zr.at[i, place_next(side, d)], onward[side][1])

    def across(i, zq):
        ref = chunk(i).at[zq, x]
        start(ref, ref, out_x.at[0], xr.at[i], pair_e)

    def tell(d):
        for side in range(2):

            @pl.when(there(side, d - 1) & onward[side][0])
            def _():
                pl.semaphore_signal(
                    ready.at[side, d - 2], inc=1, device_id=onward[side][1], device_id_type=MESH
                )

    def hear(d):
        for side in range(2):

            @pl.when(there(side, d))
            def _():
                pl.semaphore_wait(ready.at[side, d - 2], 1)

    def tiles_cross():
        start(meta.at[q, x], meta.at[q, x], out_t.at[0], xmr.at[0], pair_e)

    def tiles_out():
        arrived(meta.at[q, 1 - x], xmr.at[0])
        for d in order:
            start(meta.at[q], meta.at[q], out_t.at[0], zmr.at[0], to(a, ((q + d) % N) * 2 + x))

    def tiles_in():
        arrived(meta.at[0 : N - 1], zmr.at[0])

    def pair_step(p, d):
        if d == 0:
            arrived(cot_far.at[p, q, 1 - x], xr.at[C + p])
        for side in range(2):

            @pl.when(there(side, d) if d else onward[side][0])
            def _():
                if d:
                    arrived(cot_far.at[p, at(side, d)], zr.at[C + p, place(side, d)])
                if 0 < d < N - 1:

                    @pl.when(onward[side][0])
                    def _():
                        pass_pair(p, side, d)

                if d == 0:
                    pass_pair(p, side, d)

    def begin(i):
        for side in range(2):

            @pl.when(onward[side][0])
            def _():
                pass_cot(i, side, 0)

    def step(i, d):
        for side in range(2):

            @pl.when(there(side, d))
            def _():
                arrived(chunk(i).at[at(side, d), x], zr.at[i, place(side, d)])
                if d < N - 1:

                    @pl.when(onward[side][0])
                    def _():
                        pass_cot(i, side, d)

                if i < C:
                    across(i, at(side, d))

    def begin_far():
        arrived(cot_far.at[:, q, x], cy_r.at[0])
        for s in range(A):
            across(C + s, q)

    def cross_all(i):
        for zq in range(N):
            across(i, zq)

    complete = set()

    def gathered(i):
        if i not in complete:
            complete.add(i)
            arrived(chunk(i).at[:, 1 - x], xr.at[i])

    order = sorted(range(1, N), key=lambda d: min(d, N - d))

    def send_w(k):
        ref = wfull.at[slice(*groups[k]), mine]
        start(ref, ref, out_w.at[0], wy_r.at[k], pair_y)

    def share_w(k):
        ref = wfull.at[slice(*groups[k]), mine]
        start(ref, ref, out_w.at[0], wf_r.at[k], pair_c)

    def forward_w(k):
        ref = wfull.at[slice(*groups[k]), theirs]
        arrived(ref, wy_r.at[k])
        start(ref, ref, out_w.at[0], wf_r.at[k], pair_c)

    def send_far():
        start(
            cot_all.at[summed:C, q, x], cot_far.at[:, q, x], out_x.at[0], cy_r.at[0], pair_y
        )

    def placer(slot_row):
        return (lax.broadcasted_iota(jnp.int32, (cap, tok), 0).astype(F32) == slot_row).astype(BF16)

    eye = lax.broadcasted_iota(jnp.int32, (tok, tok), 0) == lax.broadcasted_iota(jnp.int32, (tok, tok), 1)

    def to_row(col):
        return jnp.sum(jnp.where(eye, col, 0.0), axis=0, keepdims=True)

    def to_col(row):
        return jnp.sum(jnp.where(eye, row, 0.0), axis=1, keepdims=True)

    def routes():
        upper = (
            lax.broadcasted_iota(jnp.int32, (tok, tok), 0) < lax.broadcasted_iota(jnp.int32, (tok, tok), 1)
        ).astype(BF16)
        chosen, weight = [], []
        for b in range(ne):
            tile = meta[b // 2, b % 2]
            hit = tile[0:topk, 0:tok] == e.astype(F32)
            chosen.append(jnp.sum(jnp.where(hit, 1.0, 0.0), axis=0, keepdims=True))
            weight.append(jnp.sum(jnp.where(hit, tile[topk : 2 * topk, 0:tok], 0.0), axis=0, keepdims=True))
        choose = jnp.concatenate(chosen, axis=0)
        position = jnp.dot(choose.astype(BF16), upper, preferred_element_type=F32)
        slots = jnp.where(choose > 0.0, position, -1.0)
        return [slots[b : b + 1, :] for b in range(ne)], weight

    def pick(slot_rows, gate_rows):
        for b in range(ne):
            rows_b = lax.dot_general(
                placer(slot_rows[b]), hidden[b * cap : (b + 1) * cap, :], (((0,), (0,)), ((), ())),
                preferred_element_type=F32,
            )
            ht[b // 2, b % 2] = rows_b.astype(BF16)
            gh[b // 2, b % 2] = (to_col(gate_rows[b]) * rows_b).astype(BF16)
        ght[...] = gh[...].reshape(T, F).astype(F32).T.astype(BF16)

    def send_rows():
        there_rows = pl.ds(pl.multiple_of((1 - r) * 2 * rows, 2 * rows), 2 * rows)
        start(ght.at[there_rows], ght_far, out_g.at[0], hy_r.at[0], pair_y)

    def block_of(j, b):
        return jnp.dot(ght[w_rows(b), :], cot_all[j].reshape(T, cw), preferred_element_type=F32)

    def begin_grads(j):
        gathered(j)
        for k in range(2):
            wg_send1[j, k] = block_of(j, ((r + k) % 2) * 2 + 1 - c).astype(BF16)
        start(wg_send1.at[j], wg_recv1.at[j], out_g.at[0], g1_r.at[j], pair_c)
        wg_hold[j] = block_of(j, (1 - r) * 2 + c)
        wg_own[j] = block_of(j, r * 2 + c)

    def pass_grads(j):
        arrived(wg_recv1.at[j], g1_r.at[j])
        wg_send2[j] = (wg_hold[j] + wg_recv1[j, 1].astype(F32)).astype(BF16)
        start(wg_send2.at[j], wg_recv2.at[j], out_g.at[0], g2_r.at[j], pair_y)

    def full_grads(j):
        s = j - summed
        gathered(j)
        if s >= A:
            gathered(C + s)
        if s == 0:
            arrived(ght_far, hy_r.at[0])

        def both(core):
            other = jnp.dot(
                ght_far[w_rows(core), :], cot_far[s].reshape(T, cw), preferred_element_type=F32
            )
            return block_of(j, r * 2 + core) + other

        wg_part[s] = both(1 - c).astype(BF16)
        start(wg_part.at[s], wg_recvp.at[s], out_g.at[0], g1_r.at[j], pair_c)
        wg_own[j] = both(c)

    def out_part(k):
        piece = slice(*groups[k])
        arrived(wfull.at[piece, 0 : 2 * rows], wf_r.at[k])
        if k < lined:
            for j in range(*groups[k]):
                val = jnp.dot(gh[...].reshape(T, F), wfull[j], preferred_element_type=F32)
                sum_own[j] = val.reshape(N, 2, tok, vw)
                line_step(j, 0)
            return
        lhs = gh[:, pl.ds(1 - x, 1)].reshape(N * tok, F)
        for j in range(*groups[k]):
            val = jnp.dot(lhs, wfull[j], preferred_element_type=F32)
            mx_send1[j] = val.astype(BF16).reshape(N, tok, vw)
        start(mx_send1.at[piece], mx_recv1.at[piece], out_x.at[0], m1_r.at[k - lined], pair_e)
        lhs = gh[:, pl.ds(x, 1)].reshape(N * tok, F)
        for j in range(*groups[k]):
            val = jnp.dot(lhs, wfull[j], preferred_element_type=F32)
            mx_own[j] = val.reshape(N, tok, vw)

    def z_part(k):
        for j in range(*groups[k]):
            i = j * vw // cw
            gathered(i)
            part = cot_all[i, :, :, :, cols(j % (cw // vw), vw)].reshape(T, vw)
            val = lax.dot_general(part, wfull[j], (((1,), (1,)), ((), ())), preferred_element_type=F32)
            z[...] = val if j == 0 else z[...] + val

    def line_step(j, d):
        last = N - 1 - d

        @pl.when(q == d)
        def _():
            if d:
                arrived(sum_up.at[j, d:N], up_r.at[j])
            for o in range(d + 1, N):
                total = sum_own[j, o] + sum_up[j, o].astype(F32) if d else sum_own[j, o]
                sum_send[j, o] = total.astype(BF16)
            if d < N - 1:
                piece = pl.ds(d + 1, N - 1 - d)
                start(sum_send.at[j, piece], sum_up.at[j, piece], out_x.at[0], up_r.at[j], ahead)

        @pl.when(q == last)
        def _():
            if d:
                arrived(sum_down.at[j, 0 : last + 1], down_r.at[j])
            for o in range(last):
                total = sum_own[j, o] + sum_down[j, o].astype(F32) if d else sum_own[j, o]
                sum_send[j, o] = total.astype(BF16)
            if last:
                piece = pl.ds(0, last)
                start(sum_send.at[j, piece], sum_down.at[j, piece], out_x.at[0], down_r.at[j], behind)

    def line_sum(j, xq):
        return sum_own[j, q, xq] + sum_up[j, q, xq].astype(F32) + sum_down[j, q, xq].astype(F32)

    def line_cross(j):
        sum_send2[j] = line_sum(j, 1 - x).astype(BF16)
        start(sum_send2.at[j], sum_recv2.at[j], out_x.at[0], sum_r.at[j], pair_e)

    def finish_line(j):
        arrived(sum_recv2.at[j], sum_r.at[j])
        mixed[:, cols(j, vw)] = (line_sum(j, x) + sum_recv2[j].astype(F32)).astype(BF16)

    early = groups[-2][0]

    def mix_part(k):
        piece = slice(*groups[k])
        arrived(mx_recv1.at[piece], m1_r.at[k - lined])
        sem = m2_r.at[max(0, k - len(groups) + 3)]
        for d in order:
            o = (q + d) % N
            for j in range(*groups[k]):
                mx_send2[j, o] = (mx_own[j, o] + mx_recv1[j, o].astype(F32)).astype(BF16)
            start(mx_send2.at[piece, o], mx_recv2.at[piece, q], out_x.at[0], sem, to(a, o * 2 + x))

    def hidden_part(slot_rows, gate_rows):
        for b in range(ne):
            zb = z[b * tok : (b + 1) * tok, :]
            gg_col = jnp.sum(ht[b // 2, b % 2].astype(F32) * zb, axis=1, keepdims=True)
            gg_send[b, 0:1, 0:tok] = to_row(gg_col)
            scaled = (to_col(gate_rows[b]) * zb).astype(BF16)
            hidden_grads[b * cap : (b + 1) * cap, :] = jnp.dot(
                placer(slot_rows[b]), scaled, preferred_element_type=F32
            ).astype(BF16)
        for d in range(1, ne):
            o = (e + d) % ne
            start(gg_send.at[o], gg_recv.at[e], out_gg.at[0], gg_r.at[0], to(a, o))
        gg_recv[e] = gg_send[e]

    def finish_mixed(k):
        first, last = (M, early) if k == 0 else groups[k - 3]
        arrived(mx_recv2.at[first:last, 0 : N - 1], m2_r.at[k])
        for j in range(first, last):
            total = mx_own[j, q] + mx_recv1[j, q].astype(F32)
            for d in order:
                total = total + mx_recv2[j, (q - d + N) % N].astype(F32)
            mixed[:, cols(j, vw)] = total.astype(BF16)

    def finish_gates():
        arrived(gg_recv.at[0 : ne - 1], gg_r.at[0])
        for k in range(topk):
            row = jnp.zeros((1, tok), F32)
            for b in range(ne):
                row = row + jnp.where(idf[k : k + 1, :] == float(b), gg_recv[b, 0:1, 0:tok], 0.0)
            gate_grads[k : k + 1, :] = row

    def finish_grads(j):
        if j >= summed:
            arrived(wg_recvp.at[j - summed], g1_r.at[j])
            weight_grads[:, cols(j)] = (wg_own[j] + wg_recvp[j - summed].astype(F32)).astype(BF16)
            return
        val = wg_own[j] + wg_recv1[j, 0].astype(F32)
        arrived(wg_recv2.at[j], g2_r.at[j])
        weight_grads[:, cols(j)] = (val + wg_recv2[j].astype(F32)).astype(BF16)

    tiles_cross()
    send_far()
    for k in range(len(groups)):
        send_w(k)
    for j in range(C):
        across(j, q)
    begin(0)
    begin(1)
    begin(2)
    for d in range(2, N):
        tell(d)
        if d == 2:
            for k in range(len(groups)):
                share_w(k)
        hear(d)
    tiles_out()
    begin(3)
    step(0, 1)
    step(1, 1)
    begin_far()
    begin(5)
    step(2, 1)
    step(3, 1)
    pair_step(0, 0)
    step(0, 2)
    forward_w(0)
    step(1, 2)
    own_h.wait()
    tiles_in()
    slot_rows, gate_rows = routes()
    pick(slot_rows, gate_rows)
    send_rows()
    out_part(0)
    step(2, 2)
    step(3, 2)
    step(5, 1)
    step(0, 3)
    step(1, 3)
    forward_w(1)
    out_part(1)
    line_step(0, 1)
    step(2, 3)
    line_step(1, 1)
    step(3, 3)
    pair_step(0, 1)
    forward_w(2)
    step(5, 2)
    out_part(2)
    forward_w(3)
    begin_grads(0)
    line_step(0, 2)
    forward_w(4)
    out_part(3)
    line_step(1, 2)
    pass_grads(0)
    mix_part(1)
    step(5, 3)
    forward_w(5)
    out_part(4)
    begin_grads(1)
    pair_step(0, 2)
    mix_part(2)
    z_part(0)
    out_part(5)
    cross_all(5)
    pass_grads(1)
    mix_part(3)
    z_part(1)
    z_part(2)
    z_part(3)
    z_part(4)
    z_part(5)
    hidden_part(slot_rows, gate_rows)
    line_step(0, 3)
    line_cross(0)
    mix_part(4)
    line_step(1, 3)
    line_cross(1)
    mix_part(5)
    pair_step(0, 3)
    full_grads(2)
    full_grads(3)
    for j in range(M):
        finish_line(j)
    finish_mixed(0)
    finish_gates()
    finish_grads(2)
    finish_grads(0)
    finish_mixed(1)
    finish_grads(3)
    finish_mixed(2)
    finish_grads(1)

    left(wfull.at[:, 0 : 3 * rows], out_w.at[0])
    left(wfull.at[:, 0 : 2 * rows + 2 * rows * T // D], out_g.at[0])
    once = (C * N + A + (S - A) * N + S) * tok // C + (2 * N - 1) * tok
    each = (C + S + A) * tok // C
    for inner in range(2):

        @pl.when((not_first & not_last) if inner else ~(not_first & not_last))
        def _():
            left(wfull.at[:, 0 : once + each * (N + 1 if inner else 1)], out_x.at[0])

    left(gg_recv.at[0 : 2 * N - 1], out_t.at[0])
    left(gg_send.at[0 : ne - 1], out_gg.at[0])


def store_kernel(count, *refs):
    sems = refs[-1]
    copies = [pltpu.make_async_copy(refs[i], refs[count + i], sems.at[i]) for i in range(count)]
    for copy in copies:
        copy.start()
    for copy in copies:
        copy.wait()


def fused(hidden, weight_rows, expert_ids, gates, cotangent):
    nd, ne = lax.axis_size("dp"), lax.axis_size("expert")
    rows, D = weight_rows.shape
    tok, topk = expert_ids.shape
    F = hidden.shape[1]
    T, N = ne * tok, ne // 2
    C, S, A, K, M = 4, 2, 1, 8, 2
    groups = ((0, 2), (2, 4), (4, 5), (5, 6), (6, 7), (7, 8))
    G = len(groups)
    cw, vw, summed = D // C, D // K, C - S
    vm = pltpu.VMEM
    sem = lambda *n: pltpu.SemaphoreType.DMA(tuple(max(i, 1) for i in n))
    near, far = pl.BlockSpec(memory_space=pltpu.VMEM), pl.BlockSpec(memory_space=pltpu.HBM)
    shapes = [((tok, D), BF16), ((topk, tok), F32), (hidden.shape, BF16), ((rows, D), BF16)]
    tall = -(-2 * topk // 8) * 8
    result_bytes = 2 * (tok * D + hidden.size + rows * D) + 128 * 1024
    results = pl.pallas_call(
        functools.partial(kernel, nd, ne, C, S, A, K, M, groups),
        out_shape=tuple(pltpu.VMEM(*s) for s in shapes),
        in_specs=[far] * 5,
        out_specs=(near,) * 4,
        scratch_shapes=[
            vm((topk, tok), jnp.int32), vm((topk, tok), F32), vm(hidden.shape, BF16), vm((K, F, vw), BF16), vm((C, N, 2, tok, cw), BF16),
            vm((S, N, 2, tok, cw), BF16),
            vm((N, 2, tall, 128), F32), vm((ne, 8, 128), F32), vm((ne, 8, 128), F32),
            vm((N, 2, tok, F), BF16), vm((N, 2, tok, F), BF16), vm((F, T), BF16), vm((2 * rows, T), BF16),
            vm((T, F), F32),
            vm((summed, 2, rows, cw), BF16), vm((summed, 2, rows, cw), BF16),
            vm((S, rows, cw), BF16), vm((S, rows, cw), BF16),
            vm((summed, rows, cw), BF16), vm((summed, rows, cw), BF16), vm((C, rows, cw), F32),
            vm((summed, rows, cw), F32),
            vm((K, N, tok, vw), BF16), vm((K, N, tok, vw), BF16),
            vm((K, N, tok, vw), BF16), vm((K, N, tok, vw), BF16), vm((K, N, tok, vw), F32),
            vm((M, N, 2, tok, vw), F32), vm((M, N, 2, tok, vw), BF16), vm((M, N, 2, tok, vw), BF16),
            vm((M, N, 2, tok, vw), BF16), vm((M, tok, vw), BF16), vm((M, tok, vw), BF16),
            sem(G), sem(G), sem(C + S, N - 1), sem(C + S), sem(1), sem(1), sem(1), sem(1), sem(1),
            sem(C), sem(summed), sem(G - sum(last <= M for _, last in groups)), sem(3), sem(M), sem(M), sem(M), sem(1), sem(1), sem(1), sem(1), sem(1),
            pltpu.SemaphoreType.REGULAR((2, max(N - 2, 1))),
        ],
        compiler_params=pltpu.CompilerParams(
            collective_id=0, has_side_effects=True, vmem_limit_bytes=VMEM_BYTES - result_bytes
        ),
    )(hidden, weight_rows, expert_ids.T, gates.T, cotangent)
    mixed, gate_grads, hidden_grads, sums = pl.pallas_call(
        functools.partial(store_kernel, len(shapes)),
        out_shape=tuple(jax.ShapeDtypeStruct(*s) for s in shapes),
        in_specs=[pl.BlockSpec(memory_space=pl.ANY)] * 4,
        out_specs=(far,) * 4,
        scratch_shapes=[sem(len(shapes))],
        compiler_params=pltpu.CompilerParams(vmem_limit_bytes=1024 * 1024),
    )(*results)
    return mixed, gate_grads.T, hidden_grads, sums


def slot_table(expert_ids, experts, capacity):
    flat_ids = expert_ids.reshape(-1)
    choose = (flat_ids[:, None] == jnp.arange(experts, dtype=jnp.int32)[None, :]).astype(jnp.int32)
    earlier = jnp.cumsum(choose, axis=0) - choose
    position = jnp.sum(earlier * choose, axis=1)
    target = flat_ids * capacity + position
    return (target[None, :] == jnp.arange(experts * capacity, dtype=jnp.int32)[:, None]).astype(BF16)


def plain(hidden, weight_rows, expert_ids, gates, cotangent):
    experts = lax.axis_size("expert")
    capacity = hidden.shape[0] // experts
    tok, topk = expert_ids.shape
    width = cotangent.shape[1]
    table = slot_table(expert_ids, experts, capacity)
    weight = lax.all_gather(weight_rows, "dp", axis=0, tiled=True)
    outputs = jnp.dot(hidden, weight, preferred_element_type=F32).astype(BF16)
    back = lax.all_to_all(outputs, "expert", split_axis=0, concat_axis=0, tiled=True)
    picked = lax.dot_general(table, back, (((0,), (0,)), ((), ())), preferred_element_type=F32)
    picked = picked.reshape(tok, topk, width)
    cot32 = cotangent.astype(F32)[:, None, :]
    mixed = jnp.sum(gates[:, :, None] * picked, axis=1).astype(BF16)
    gate_grads = jnp.sum(picked * cot32, axis=2)
    routed = (gates[:, :, None] * cot32).astype(BF16).reshape(-1, width)
    packed = jnp.dot(table, routed, preferred_element_type=F32).astype(BF16)
    grads = lax.all_to_all(packed, "expert", split_axis=0, concat_axis=0, tiled=True)
    hidden_grads = lax.dot_general(
        grads, weight, (((1,), (1,)), ((), ())), preferred_element_type=F32
    ).astype(BF16)
    partial = lax.dot_general(
        hidden, grads, (((0,), (0,)), ((), ())), preferred_element_type=F32
    ).astype(BF16)
    sums = lax.psum_scatter(partial, "dp", scatter_dimension=0, tiled=True)
    return mixed, gate_grads, hidden_grads, sums


def per_device(hidden, w_down, expert_ids, gates, cotangent):
    nd, ne = lax.axis_size("dp"), lax.axis_size("expert")
    rows, width = w_down.shape[1:]
    cap, tok = hidden.shape[0] // ne, expert_ids.shape[0]
    tiled = rows % 16 == 0 and cap % 16 == 0 and tok % 16 == 0 and tok <= 128
    paired = nd == 4 and ne % 2 == 0 and width % 512 == 0
    small = expert_ids.shape[1] <= 8
    body = fused if tiled and paired and small else plain
    mixed, gate_grads, hidden_grads, sums = body(
        hidden, w_down.reshape(rows, width), expert_ids, gates, cotangent
    )
    return mixed, gate_grads, hidden_grads, sums.reshape(1, rows, width)


def solution(mesh):
    split = P(("dp", "expert"), None)
    weights = P("expert", "dp", None)
    return jax.shard_map(
        per_device,
        mesh=mesh,
        in_specs=(split, weights, split, split, split),
        out_specs=(split, split, split, weights),
        check_vma=False,
    )
```
